32 devices in a mesh: seq: 4 (over x, core), mlp: 4 (over z), head: 2 (over y).
Axes of the slice: x: 2, y: 2, z: 4, core: 2. Of those that a mesh axis runs over, the one named last changes fastest.
Arguments:
- tokens: bfloat16 [4096, 2048], P(('seq', 'mlp', 'head')), may hold values from -6 to 6
- cotangent: bfloat16 [4096, 2048], P(('seq', 'mlp', 'head')), may hold values from -6 to 6
- attention_in: float32 [2048, 6144], P('seq', ('mlp', 'head')), may hold values from -0.15467961 to 0.15467961
- feedforward_in: float32 [2048, 12288], P('seq', ('mlp', 'head')), may hold values from -0.15467961 to 0.15467961
- projection_out: float32 [8192, 2048], P(('mlp', 'head'), 'seq'), may hold values from -0.87 to 0.87
- attention_mean: float32 [2048, 6144], P('seq', ('mlp', 'head')), may hold values from -98.56 to 98.56
- feedforward_mean: float32 [2048, 12288], P('seq', ('mlp', 'head')), may hold values from -24.96 to 24.96
- projection_mean: float32 [8192, 2048], P(('mlp', 'head'), 'seq'), may hold values from -30.08 to 30.08
- attention_power: float32 [2048, 6144], P('seq', ('mlp', 'head')), may hold values from 1.024 to 65.536
- feedforward_power: float32 [2048, 12288], P('seq', ('mlp', 'head')), may hold values from 1.024 to 4.096
- projection_power: float32 [8192, 2048], P(('mlp', 'head'), 'seq'), may hold values from 0.16384 to 5.89824
- gains: float32 [4352], replicated, may hold values from 0.8 to 2
- gain_mean: float32 [4352], replicated, may hold values from -115.2 to 115.2
- gain_power: float32 [4352], replicated, may hold values from 4.096 to 262.144
- document_lengths: int32 [4, 8], P('seq'), may hold values from 1 to 512, 1024 in all within a row
- step_count: int32 [1], replicated, may hold values from 2 to 20
Outputs:
- block_output: bfloat16 [4096, 2048], P(('seq', 'mlp', 'head'))
- input_gradient: float32 [4096, 2048], P(('seq', 'mlp', 'head'))
- attention_master: float32 [2048, 6144], P('seq', ('mlp', 'head'))
- feedforward_master: float32 [2048, 12288], P('seq', ('mlp', 'head'))
- projection_master: float32 [8192, 2048], P(('mlp', 'head'), 'seq')
- mean_attention: float32 [2048, 6144], P('seq', ('mlp', 'head'))
- mean_feedforward: float32 [2048, 12288], P('seq', ('mlp', 'head'))
- mean_projection: float32 [8192, 2048], P(('mlp', 'head'), 'seq')
- power_attention: float32 [2048, 6144], P('seq', ('mlp', 'head'))
- power_feedforward: float32 [2048, 12288], P('seq', ('mlp', 'head'))
- power_projection: float32 [8192, 2048], P(('mlp', 'head'), 'seq')
- attention_copy: bfloat16 [2048, 6144], P('seq', ('mlp', 'head'))
- feedforward_copy: bfloat16 [2048, 12288], P('seq', ('mlp', 'head'))
- projection_copy: bfloat16 [8192, 2048], P(('mlp', 'head'), 'seq')
- gains_next: float32 [4352], replicated
- mean_gains: float32 [4352], replicated
- power_gains: float32 [4352], replicated
- matrix_norms: float32 [2, 8], replicated
The draws below stay inside these ranges and needn't reach their ends.
Inputs may be any that keep to these rules, and one draw needn't show every extreme that they name: `document_lengths`: row s lists, in order, the lengths of the 8 documents packed into sequence s; each row sums to 1024, and its longest document has exactly 512 tokens.
All inputs are finite; a program needn't handle non-finite values.
Results may differ from the reference program's by a relative error of at most 0.022.
Values may be sent and summed in bfloat16 or wider, within the bound.
A program may use at most 192 MiB of HBM per device.

```python
import math
import jax
import jax.numpy as jnp
import numpy as np
from jax import lax

MODEL_DIM = 2048
HQ = 16
KEY_VALUE_HEADS = 8
HEAD_SIZE = 128
HIDDEN_UNITS = 6144
SEQUENCE_LENGTH = 1024
DOCS = 8
QUERY_PER_KEY = 2
GROUP_ATTN_COLS = 768
GATE_UP_COLS = 1536
GROUP_OUT_ROWS = 1024
GAIN_LEN = 4352
DOC_MOST = 512
SEQS = 4
TOKEN_COUNT = 4096
N_SEQ = 4


gradient_factors = (1.0, 1.0, 2.0, 0.5, 0.5, 0.5, 0.2, 0.6)


def random_signs(key, shape):
    return jnp.clip(jax.random.normal(key, shape, jnp.float32), -4.0, 4.0)


def dispersion_factor(key, shape):
    return jnp.exp(jax.random.uniform(key, shape, jnp.float32, 0.0, math.log(4.0)))


def increasing(item_count):
    return jnp.exp((jnp.arange(item_count, dtype=jnp.float32) / item_count - 0.5) * math.log(3.0))


def attention_classes_sampled(item_count, group_cols, query_cols, head_width):
    column = jnp.arange(item_count, dtype=jnp.int32) % group_cols
    return jnp.where(column < query_cols, 0, jnp.where(column < query_cols + head_width, 1, jnp.where(column < query_cols + 2 * head_width, 2, 3))).astype(jnp.int32)


def forward_classes_sampled(item_count, group_cols):
    column = jnp.arange(item_count, dtype=jnp.int32) % group_cols
    return (4 + (column >= group_cols // 2).astype(jnp.int32)).astype(jnp.int32)


def output_classes_sampled(item_count, group_rows, query_cols):
    row_index = jnp.arange(item_count, dtype=jnp.int32) % group_rows
    return (6 + (row_index >= query_cols).astype(jnp.int32)).astype(jnp.int32)


def selection_factor(class_index):
    factor_table = jnp.array(gradient_factors, jnp.float32)
    chosen = (class_index[:, None] == jnp.arange(8, dtype=jnp.int32)[None, :]).astype(jnp.float32)
    return jnp.sum(chosen * factor_table[None, :], axis=1)


def draw_attention_in(key, part):
    return random_signs(key, (MODEL_DIM, KEY_VALUE_HEADS * GROUP_ATTN_COLS)) * (increasing(MODEL_DIM) / MODEL_DIM ** 0.5)[:, None]


def draw_feedforward_in(key, part):
    return random_signs(key, (MODEL_DIM, KEY_VALUE_HEADS * GATE_UP_COLS)) * (increasing(MODEL_DIM) / MODEL_DIM ** 0.5)[:, None]


def draw_projection_out(key, part):
    class_index = output_classes_sampled(KEY_VALUE_HEADS * GROUP_OUT_ROWS, GROUP_OUT_ROWS, QUERY_PER_KEY * HEAD_SIZE)
    scale_per_row = jnp.where(class_index == 6, 0.125, HIDDEN_UNITS ** (-0.5))
    return random_signs(key, (KEY_VALUE_HEADS * GROUP_OUT_ROWS, MODEL_DIM)) * scale_per_row[:, None] * increasing(MODEL_DIM)[None, :]


def draw_attention_mean(key, part):
    scale_per_column = selection_factor(attention_classes_sampled(KEY_VALUE_HEADS * GROUP_ATTN_COLS, GROUP_ATTN_COLS, QUERY_PER_KEY * HEAD_SIZE, HEAD_SIZE)) * TOKEN_COUNT ** 0.5
    return random_signs(key, (MODEL_DIM, KEY_VALUE_HEADS * GROUP_ATTN_COLS)) * 0.111 * scale_per_column[None, :] * increasing(MODEL_DIM)[:, None]


def draw_feedforward_mean(key, part):
    scale_per_column = selection_factor(forward_classes_sampled(KEY_VALUE_HEADS * GATE_UP_COLS, GATE_UP_COLS)) * TOKEN_COUNT ** 0.5
    return random_signs(key, (MODEL_DIM, KEY_VALUE_HEADS * GATE_UP_COLS)) * 0.111 * scale_per_column[None, :] * increasing(MODEL_DIM)[:, None]


def draw_projection_mean(key, part):
    scale_per_row = selection_factor(output_classes_sampled(KEY_VALUE_HEADS * GROUP_OUT_ROWS, GROUP_OUT_ROWS, QUERY_PER_KEY * HEAD_SIZE)) * TOKEN_COUNT ** 0.5
    return random_signs(key, (KEY_VALUE_HEADS * GROUP_OUT_ROWS, MODEL_DIM)) * 0.111 * scale_per_row[:, None] * increasing(MODEL_DIM)[None, :]


def draw_attention_power(key, part):
    scale_per_column = selection_factor(attention_classes_sampled(KEY_VALUE_HEADS * GROUP_ATTN_COLS, GROUP_ATTN_COLS, QUERY_PER_KEY * HEAD_SIZE, HEAD_SIZE))
    return dispersion_factor(key, (MODEL_DIM, KEY_VALUE_HEADS * GROUP_ATTN_COLS)) * 0.001 * TOKEN_COUNT * (scale_per_column * scale_per_column)[None, :]


def draw_feedforward_power(key, part):
    scale_per_column = selection_factor(forward_classes_sampled(KEY_VALUE_HEADS * GATE_UP_COLS, GATE_UP_COLS))
    return dispersion_factor(key, (MODEL_DIM, KEY_VALUE_HEADS * GATE_UP_COLS)) * 0.001 * TOKEN_COUNT * (scale_per_column * scale_per_column)[None, :]


def draw_projection_power(key, part):
    scale_per_row = selection_factor(output_classes_sampled(KEY_VALUE_HEADS * GROUP_OUT_ROWS, GROUP_OUT_ROWS, QUERY_PER_KEY * HEAD_SIZE))
    return dispersion_factor(key, (KEY_VALUE_HEADS * GROUP_OUT_ROWS, MODEL_DIM)) * 0.001 * TOKEN_COUNT * (scale_per_row * scale_per_row)[:, None]


def gain_scale():
    index_all = jnp.arange(GAIN_LEN, dtype=jnp.int32)
    return jnp.where(index_all < 2 * MODEL_DIM, TOKEN_COUNT ** 0.5, (TOKEN_COUNT * HQ) ** 0.5)


def draw_gains(key, part):
    index_all = jnp.arange(GAIN_LEN, dtype=jnp.int32)
    near_one = 1.0 + 0.2 * jax.random.uniform(jax.random.fold_in(key, 1), (GAIN_LEN,), jnp.float32, -1.0, 1.0)
    above_one = jax.random.uniform(jax.random.fold_in(key, 2), (GAIN_LEN,), jnp.float32, 1.0, 2.0)
    return jnp.where(index_all < 2 * MODEL_DIM, near_one, above_one)


def draw_gain_mean(key, part):
    return random_signs(key, (GAIN_LEN,)) * 0.111 * gain_scale()


def draw_gain_power(key, part):
    scale_all = gain_scale()
    return dispersion_factor(key, (GAIN_LEN,)) * 0.001 * scale_all * scale_all


def block_levels(key, shape, split, smallest, high):
    def one(dim, parts):
        heights = jax.random.uniform(jax.random.fold_in(jax.random.fold_in(key, 6), dim), (parts,), jnp.float32, smallest / len(split), high / len(split))
        return jnp.repeat(jnp.exp(heights), shape[dim] // parts).reshape((-1,) + (1,) * (len(shape) - dim - 1))

    level = one(*split[0])
    for cut in split[1:]:
        level = level * one(*cut)
    return level


def split_up(amount, total, limit, skew):
    portions = [(1 << 20) // math.isqrt(rank ** skew) + 1 for rank in range(2, amount + 1)]
    spare, holding = total - limit - (amount - 1), [1] * (amount - 1)
    while spare > 0:
        movable = [i for i in range(amount - 1) if holding[i] < limit]
        mass, budget = sum([portions[i] for i in movable]), spare
        for i in movable:
            extra = min(limit - holding[i], max(1, budget * portions[i] // mass), spare)
            holding[i] = holding[i] + extra
            spare = spare - extra
    return np.array([limit] + holding)


def uneven(own_key, amount, total, reach, slope):
    if amount == 2:
        one = jax.random.randint(own_key, (), max(1, total - reach), min(reach, total - 1) + 1)
        return jnp.stack([one, total - one])
    tallies = jnp.asarray(split_up(amount, total, reach, slope), jnp.int32)
    couples = (amount - 1) // 2
    giver, taker = tallies[1:1 + 2 * couples:2], tallies[2:2 + 2 * couples:2]
    margin = jnp.minimum(giver - 1, reach - taker)
    shifted = jax.random.randint(jax.random.fold_in(own_key, 1), (couples,), 0, 1 << 20) % (margin + 1)
    tallies = tallies.at[1:1 + 2 * couples:2].set(giver - shifted).at[2:2 + 2 * couples:2].set(taker + shifted)
    return tallies[jax.random.permutation(jax.random.fold_in(own_key, 2), amount)]


def bell_draw(rng, dims, deviation, reach, shards=(), kind=jnp.bfloat16):
    values = deviation * jax.random.normal(rng, dims, jnp.float32)
    if shards:
        values = values * block_levels(rng, dims, shards, -0.22, 0.18)
    return jnp.clip(values, -reach, reach).astype(kind)


def setup_inputs(seed: int = 0) -> dict:
    splits = jax.random.split(jax.random.key(seed), 17)
    tokens = bell_draw(splits[0], (TOKEN_COUNT, MODEL_DIM), 1.0, 6.0, ((0, 32),))
    cotangent = bell_draw(splits[1], (TOKEN_COUNT, MODEL_DIM), 1.0, 6.0, ((0, 32),))
    attention_in = draw_attention_in(jax.random.fold_in(splits[16], 71), 0)
    feedforward_in = draw_feedforward_in(jax.random.fold_in(splits[16], 71), 0)
    projection_out = draw_projection_out(jax.random.fold_in(splits[16], 71), 0)
    attention_mean = draw_attention_mean(jax.random.fold_in(splits[16], 71), 0)
    feedforward_mean = draw_feedforward_mean(jax.random.fold_in(splits[16], 71), 0)
    projection_mean = draw_projection_mean(jax.random.fold_in(splits[16], 71), 0)
    attention_power = draw_attention_power(jax.random.fold_in(splits[16], 71), 0)
    feedforward_power = draw_feedforward_power(jax.random.fold_in(splits[16], 71), 0)
    projection_power = draw_projection_power(jax.random.fold_in(splits[16], 71), 0)
    gains = draw_gains(jax.random.fold_in(splits[16], 71), 0)
    gain_mean = draw_gain_mean(jax.random.fold_in(splits[16], 71), 0)
    gain_power = draw_gain_power(jax.random.fold_in(splits[16], 71), 0)
    document_lengths = jax.vmap(lambda own: uneven(own, DOCS, SEQUENCE_LENGTH, DOC_MOST, 2))(jax.random.split(splits[14], SEQS)).reshape((SEQS, DOCS)).astype(jnp.int32)
    step_count = jax.random.randint(splits[15], (1,), 2, 21).astype(jnp.int32)
    return {"tokens": tokens, "cotangent": cotangent, "attention_in": attention_in, "feedforward_in": feedforward_in, "projection_out": projection_out, "attention_mean": attention_mean, "feedforward_mean": feedforward_mean, "projection_mean": projection_mean, "attention_power": attention_power, "feedforward_power": feedforward_power, "projection_power": projection_power, "gains": gains, "gain_mean": gain_mean, "gain_power": gain_power, "document_lengths": document_lengths, "step_count": step_count}


@jax.custom_vjp
def reduced_value(v):
    return lax.optimization_barrier(v.astype(jnp.bfloat16)).astype(jnp.float32)

@jax.custom_vjp
def reduced_backward(v):
    return v

def low_keep(v):
    return (reduced_value(v), None)

def low_pass(kept, grad):
    return (grad,)

def back_keep(v):
    return (v, None)

def back_low(kept, grad):
    return (reduced_value(grad),)
reduced_value.defvjp(low_keep, low_pass)
reduced_backward.defvjp(back_keep, back_low)
norm_epsilon = 1e-06
rope_base = 1000000.0
beta_one = 0.9
beta_two = 0.999
adam_epsilon = 1e-08
decay_rate = 0.01
learn_rate = 0.3
masked_score = -1e+30
highest_precision = lax.Precision.HIGHEST

def scaled_norm(values, norm_gain):
    return values * lax.rsqrt(lax.optimization_barrier(jnp.mean(values * values, axis=-1, keepdims=True)) + norm_epsilon) * norm_gain

def rotate(values, cosine_table, sine_table):
    middle = values.shape[-1] // 2
    front_half = values[..., :middle]
    back_half = values[..., middle:]
    return jnp.concatenate([front_half * cosine_table - back_half * sine_table, back_half * cosine_table + front_half * sine_table], axis=-1)

def rotary_tables(position, head_width):
    middle = head_width // 2
    frequency = jnp.exp(-(2.0 * jnp.arange(middle, dtype=jnp.float32) / head_width) * math.log(rope_base))
    angles = position.astype(jnp.float32)[:, None] * frequency[None, :]
    return (jnp.cos(angles), jnp.sin(angles))

def document_layout(lengths, total_rows):
    end_points = jnp.cumsum(lengths.astype(jnp.int32)).astype(jnp.int32)
    row_index = jnp.arange(total_rows, dtype=jnp.int32)
    passed = (row_index[:, None] >= end_points[None, :]).astype(jnp.int32)
    segment = lax.optimization_barrier(jnp.sum(passed, axis=1)).astype(jnp.int32)
    offset = lax.optimization_barrier(jnp.sum(passed * lengths.astype(jnp.int32)[None, :], axis=1)).astype(jnp.int32)
    return (segment, row_index - offset)

def attention_classes(item_count, group_cols, query_cols, head_width):
    column = jnp.arange(item_count, dtype=jnp.int32) % group_cols
    return jnp.where(column < query_cols, 0, jnp.where(column < query_cols + head_width, 1, jnp.where(column < query_cols + 2 * head_width, 2, 3))).astype(jnp.int32)

def forward_classes(item_count, group_cols):
    column = jnp.arange(item_count, dtype=jnp.int32) % group_cols
    return (4 + (column >= group_cols // 2).astype(jnp.int32)).astype(jnp.int32)

def output_classes(item_count, group_rows, query_cols):
    row_index = jnp.arange(item_count, dtype=jnp.int32) % group_rows
    return (6 + (row_index >= query_cols).astype(jnp.int32)).astype(jnp.int32)

def indicator_matrix(class_index):
    return (class_index[:, None] == jnp.arange(8, dtype=jnp.int32)[None, :]).astype(jnp.float32)

def kind_sums(matrix, kind_table, over_axis):
    return jnp.dot(lax.optimization_barrier(jnp.sum(matrix * matrix, axis=over_axis)), kind_table, precision=highest_precision)

def adam_terms(weight, gradient, first_moment, second_moment, correct_one, correct_two, decay_weight):
    first_new = beta_one * first_moment + (1.0 - beta_one) * gradient
    second_new = beta_two * second_moment + (1.0 - beta_two) * gradient * gradient
    direction = first_new / correct_one / (jnp.sqrt(second_new / correct_two) + adam_epsilon) + decay_weight * weight
    return (first_new, second_new, direction)

def one_sequence(sequence_rows, lengths, attention_reduced, forward_reduced, output_reduced, gain_vector):
    gain_one = gain_vector[:MODEL_DIM]
    gain_two = gain_vector[MODEL_DIM:2 * MODEL_DIM]
    gain_query = gain_vector[2 * MODEL_DIM:2 * MODEL_DIM + HEAD_SIZE]
    gain_key = gain_vector[2 * MODEL_DIM + HEAD_SIZE:]
    segment, position = document_layout(lengths, SEQUENCE_LENGTH)
    cosine_table, sine_table = rotary_tables(position, HEAD_SIZE)
    normed_input = reduced_value(scaled_norm(sequence_rows, gain_one))
    projected_rows = reduced_backward(jnp.dot(normed_input, attention_reduced, precision=highest_precision)).reshape(SEQUENCE_LENGTH, KEY_VALUE_HEADS, GROUP_ATTN_COLS)
    query_rows = projected_rows[:, :, :QUERY_PER_KEY * HEAD_SIZE].reshape(SEQUENCE_LENGTH, KEY_VALUE_HEADS, QUERY_PER_KEY, HEAD_SIZE)
    keys_raw = projected_rows[:, :, QUERY_PER_KEY * HEAD_SIZE:(QUERY_PER_KEY + 1) * HEAD_SIZE]
    values_low = reduced_value(projected_rows[:, :, (QUERY_PER_KEY + 1) * HEAD_SIZE:(QUERY_PER_KEY + 2) * HEAD_SIZE])
    gate_scores_raw = projected_rows[:, :, (QUERY_PER_KEY + 2) * HEAD_SIZE:]
    query_low = reduced_value(rotate(scaled_norm(query_rows, gain_query), cosine_table[:, None, None, :], sine_table[:, None, None, :]))
    key_low = reduced_value(rotate(scaled_norm(keys_raw, gain_key), cosine_table[:, None, :], sine_table[:, None, :]))
    block_rows = min(512, SEQUENCE_LENGTH)
    scaling = HEAD_SIZE ** (-0.5)
    key_index = jnp.arange(SEQUENCE_LENGTH, dtype=jnp.int32)

    def attend_tokens(begin_row):
        query_block = lax.dynamic_slice_in_dim(query_low, begin_row, block_rows, 0)
        scores = reduced_backward(jnp.einsum('qgpd,kgd->gpqk', query_block, key_low, precision=highest_precision) * scaling)
        row_index = begin_row + jnp.arange(block_rows, dtype=jnp.int32)
        segment_rows = lax.dynamic_slice_in_dim(segment, begin_row, block_rows, 0)
        visible = (segment_rows[:, None] == segment[None, :]) & (key_index[None, :] <= row_index[:, None])
        scores = jnp.where(visible, scores, masked_score)
        row_max = lax.optimization_barrier(jnp.max(scores, axis=-1, keepdims=True))
        powers = jnp.exp(scores - row_max)
        softmax_low = reduced_value(powers / lax.optimization_barrier(jnp.sum(powers, axis=-1, keepdims=True)))
        return jnp.einsum('gpqk,kgd->qgpd', softmax_low, values_low, precision=highest_precision)
    starting_rows = (jnp.arange(SEQUENCE_LENGTH // block_rows, dtype=jnp.int32) * block_rows).astype(jnp.int32)
    attended_rows = lax.map(jax.checkpoint(attend_tokens), starting_rows).reshape(SEQUENCE_LENGTH, KEY_VALUE_HEADS, QUERY_PER_KEY * HEAD_SIZE)
    attended_rows = reduced_backward(attended_rows)
    gated_hidden = reduced_value(attended_rows * jax.nn.sigmoid(gate_scores_raw)).reshape(SEQUENCE_LENGTH, KEY_VALUE_HEADS * QUERY_PER_KEY * HEAD_SIZE)
    grouped_rows = output_reduced.reshape(KEY_VALUE_HEADS, GROUP_OUT_ROWS, MODEL_DIM)
    mixing_rows = grouped_rows[:, :QUERY_PER_KEY * HEAD_SIZE].reshape(KEY_VALUE_HEADS * QUERY_PER_KEY * HEAD_SIZE, MODEL_DIM)
    down_rows = grouped_rows[:, QUERY_PER_KEY * HEAD_SIZE:].reshape(HIDDEN_UNITS, MODEL_DIM)
    middle = sequence_rows + reduced_backward(jnp.dot(gated_hidden, mixing_rows, precision=highest_precision))
    normed_second = reduced_value(scaled_norm(middle, gain_two))
    gate_up_product = reduced_backward(jnp.dot(normed_second, forward_reduced, precision=highest_precision)).reshape(SEQUENCE_LENGTH, KEY_VALUE_HEADS, GATE_UP_COLS)
    hidden_rows = HIDDEN_UNITS // KEY_VALUE_HEADS
    activated = reduced_value(jax.nn.silu(gate_up_product[:, :, :hidden_rows]) * gate_up_product[:, :, hidden_rows:]).reshape(SEQUENCE_LENGTH, HIDDEN_UNITS)
    return middle + reduced_backward(jnp.dot(activated, down_rows, precision=highest_precision))

def forward(inputs, lengths_all, attention_weight, feed_weight, output_weight, gain_vector):
    attention_reduced = reduced_value(attention_weight)
    forward_reduced = reduced_value(feed_weight)
    output_reduced = reduced_value(output_weight)
    sequences = inputs.reshape(N_SEQ, SEQUENCE_LENGTH, MODEL_DIM)

    def scan_step(carry_in, sequence_item):
        result = jax.checkpoint(one_sequence)(sequence_item[0], sequence_item[1], attention_reduced, forward_reduced, output_reduced, gain_vector)
        return (carry_in, result)
    unused, results = lax.scan(scan_step, jnp.int32(0), (sequences, lengths_all))
    return results.reshape(N_SEQ * SEQUENCE_LENGTH, MODEL_DIM)

def reference(tokens, cotangent, attention_in, feedforward_in, projection_out, attention_mean, feedforward_mean, projection_mean, attention_power, feedforward_power, projection_power, gains, gain_mean, gain_power, document_lengths, step_count):

    def layer(inputs, attention_weight, feed_weight, output_weight, gain_vector):
        return forward(inputs, document_lengths, attention_weight, feed_weight, output_weight, gain_vector)
    outputs, pullback = jax.vjp(layer, tokens.astype(jnp.float32), attention_in, feedforward_in, projection_out, gains)
    input_gradient, attention_delta, feed_delta, output_delta, gain_delta = pullback(cotangent.astype(jnp.float32))
    steps_done = step_count[0].astype(jnp.float32)
    correct_one = 1.0 - jnp.power(beta_one, steps_done)
    correct_two = 1.0 - jnp.power(beta_two, steps_done)
    mean_attention, power_attention, move_attention = adam_terms(attention_in, attention_delta, attention_mean, attention_power, correct_one, correct_two, decay_rate)
    mean_feedforward, power_feedforward, move_feed = adam_terms(feedforward_in, feed_delta, feedforward_mean, feedforward_power, correct_one, correct_two, decay_rate)
    mean_projection, power_projection, move_output = adam_terms(projection_out, output_delta, projection_mean, projection_power, correct_one, correct_two, decay_rate)
    attention_lookup = indicator_matrix(attention_classes(KEY_VALUE_HEADS * GROUP_ATTN_COLS, GROUP_ATTN_COLS, QUERY_PER_KEY * HEAD_SIZE, HEAD_SIZE))
    forward_lookup = indicator_matrix(forward_classes(KEY_VALUE_HEADS * GATE_UP_COLS, GATE_UP_COLS))
    output_lookup = indicator_matrix(output_classes(KEY_VALUE_HEADS * GROUP_OUT_ROWS, GROUP_OUT_ROWS, QUERY_PER_KEY * HEAD_SIZE))
    weight_squares = kind_sums(attention_in, attention_lookup, 0) + kind_sums(feedforward_in, forward_lookup, 0) + kind_sums(projection_out, output_lookup, 1)
    update_squares = kind_sums(move_attention, attention_lookup, 0) + kind_sums(move_feed, forward_lookup, 0) + kind_sums(move_output, output_lookup, 1)
    trust_ratio = jnp.sqrt(weight_squares) / jnp.sqrt(update_squares)
    attention_master = attention_in - learn_rate * jnp.dot(attention_lookup, trust_ratio, precision=highest_precision)[None, :] * move_attention
    feedforward_master = feedforward_in - learn_rate * jnp.dot(forward_lookup, trust_ratio, precision=highest_precision)[None, :] * move_feed
    projection_master = projection_out - learn_rate * jnp.dot(output_lookup, trust_ratio, precision=highest_precision)[:, None] * move_output
    mean_gains, power_gains, move_gains = adam_terms(gains, gain_delta, gain_mean, gain_power, correct_one, correct_two, 0.0)
    gains_next = gains - learn_rate * move_gains
    matrix_norms = jnp.stack([jnp.sqrt(weight_squares), jnp.sqrt(update_squares)])
    return (outputs.astype(jnp.bfloat16), input_gradient, attention_master, feedforward_master, projection_master, mean_attention, mean_feedforward, mean_projection, power_attention, power_feedforward, power_projection, attention_master.astype(jnp.bfloat16), feedforward_master.astype(jnp.bfloat16), projection_master.astype(jnp.bfloat16), gains_next, mean_gains, power_gains, matrix_norms)
```

```python
import functools
import math

import jax
import jax.numpy as jnp
from jax import lax
from jax.experimental import pallas as pl
from jax.experimental.pallas import tpu as pltpu
from jax.sharding import PartitionSpec as P

norm_epsilon = 1e-06
rope_base = 1000000.0
beta_one = 0.9
beta_two = 0.999
adam_epsilon = 1e-08
decay_rate = 0.01
learn_rate = 0.3
masked_score = -1e30
highest_precision = lax.Precision.HIGHEST
MESH = pl.DeviceIdType.MESH


def remote(src, dst, ssem, rsem, dev):
    return pltpu.make_async_remote_copy(src_ref=src, dst_ref=dst, send_sem=ssem, recv_sem=rsem, device_id=dev, device_id_type=MESH)

def enter(Z, z, y):
    bar = pltpu.get_barrier_semaphore()
    pl.semaphore_signal(bar, inc=1, device_id={"head": 1 - y}, device_id_type=MESH)
    @pl.when(z > 0)
    def _():
        pl.semaphore_signal(bar, inc=1, device_id={"mlp": z - 1}, device_id_type=MESH)
    @pl.when(z < Z - 1)
    def _():
        pl.semaphore_signal(bar, inc=1, device_id={"mlp": z + 1}, device_id_type=MESH)
    inner = (z > 0) & (z < Z - 1)
    @pl.when(inner)
    def _(): pl.semaphore_wait(bar, 3)
    @pl.when(jnp.logical_not(inner))
    def _(): pl.semaphore_wait(bar, 2)

def ag_kernel(Z, C, x_ref, out_ref, usem, dsem, ysem, rsem):
    z = lax.axis_index("mlp"); y = lax.axis_index("head")
    R = x_ref.shape[0]; r = R // C
    enter(Z, z, y)
    own = z * 2 + y
    def cp(src, b, c, sem, dev):
        return remote(src, out_ref.at[b, pl.ds(c * r, r)], sem, rsem.at[b, c], dev)
    def blk(b, c): return out_ref.at[b, pl.ds(c * r, r)]
    def up(src, b, zb, c): return cp(src, b, c, usem.at[zb, c], {"mlp": z + 1})
    def dn(src, b, zb, c): return cp(src, b, c, dsem.at[zb, c], {"mlp": z - 1})
    def yy(src, b, zb, c): return cp(src, b, c, ysem.at[zb, c], {"head": 1 - y})
    for c in range(C):
        s = x_ref.at[pl.ds(c * r, r)]
        @pl.when(z < Z - 1)
        def _(): up(s, own, z, c).start()
        @pl.when(z > 0)
        def _(): dn(s, own, z, c).start()
        yy(s, own, z, c).start()
    out_ref[own] = x_ref[...]
    for k in range(1, Z):
        for c in range(C):
            @pl.when(z - k >= 0)
            def _():
                zb = z - k; b = zb * 2 + y
                yy(blk(b, c), b, zb, c).wait_recv()
                @pl.when(z < Z - 1)
                def _(): up(blk(b, c), b, zb, c).start()
                yy(blk(b, c), b, zb, c).start()
            @pl.when(z + k <= Z - 1)
            def _():
                zb = z + k; b = zb * 2 + y
                yy(blk(b, c), b, zb, c).wait_recv()
                @pl.when(z > 0)
                def _(): dn(blk(b, c), b, zb, c).start()
                yy(blk(b, c), b, zb, c).start()
    for zb in range(Z):
        for c in range(C):
            b = zb * 2 + (1 - y)
            yy(blk(b, c), b, zb, c).wait_recv()
    for zb in range(Z):
        for c in range(C):
            b = zb * 2 + y
            yy(blk(b, c), b, zb, c).wait_send()
            @pl.when((z < Z - 1) & (zb <= z))
            def _(): up(blk(b, c), b, zb, c).wait_send()
            @pl.when((z > 0) & (zb >= z))
            def _(): dn(blk(b, c), b, zb, c).wait_send()

def ag(x, Z, C, cid=1):
    R, D = x.shape
    return pl.pallas_call(functools.partial(ag_kernel, Z, C),
        out_shape=jax.ShapeDtypeStruct((2 * Z, R, D), x.dtype),
        in_specs=[pl.BlockSpec(memory_space=pltpu.VMEM)], out_specs=pl.BlockSpec(memory_space=pltpu.VMEM),
        scratch_shapes=[pltpu.SemaphoreType.DMA((Z, C))] * 3 + [pltpu.SemaphoreType.DMA((2 * Z, C))],
        compiler_params=pltpu.CompilerParams(collective_id=cid, has_side_effects=True, vmem_limit_bytes=60 << 20))(x)

def rs_kernel(Z, C, p_ref, out_ref, ybuf, bbuf, abuf, ubuf, dbuf, ysem, usem, dsem, yr, br, ar):
    z = lax.axis_index("mlp"); y = lax.axis_index("head")
    R, D = out_ref.shape; r = R // C
    enter(Z, z, y)
    def rows(c): return pl.ds(c * r, r)
    def yy(zb, c): return remote(p_ref.at[zb * 2 + 1 - y, rows(c)], ybuf.at[zb, rows(c)], ysem.at[zb, c], yr.at[zb, c], {"head": 1 - y})
    def up(zb, c): return remote(ubuf.at[zb, rows(c)], bbuf.at[zb, rows(c)], usem.at[zb, c], br.at[zb, c], {"mlp": z + 1})
    def dn(zb, c): return remote(dbuf.at[zb, rows(c)], abuf.at[zb, rows(c)], dsem.at[zb, c], ar.at[zb, c], {"mlp": z - 1})
    for k in range(Z - 1, -1, -1):
        for c in range(C):
            @pl.when(z + k <= Z - 1)
            def _(): yy(z + k, c).start()
            if k:
                @pl.when(z - k >= 0)
                def _(): yy(z - k, c).start()
    f = lambda v: v.astype(jnp.float32)
    def own(zb, c): return f(p_ref[zb * 2 + y, rows(c)]) + f(ybuf[zb, rows(c)])
    for k in range(Z - 1, 0, -1):
        for c in range(C):
            @pl.when(z + k <= Z - 1)
            def _():
                zb = z + k
                yy(zb, c).wait_recv()
                @pl.when(z > 0)
                def _():
                    up(zb, c).wait_recv()
                    ubuf[zb, rows(c)] = (own(zb, c) + f(bbuf[zb, rows(c)])).astype(ubuf.dtype)
                @pl.when(z == 0)
                def _():
                    ubuf[zb, rows(c)] = own(zb, c).astype(ubuf.dtype)
                up(zb, c).start()
            @pl.when(z - k >= 0)
            def _():
                zb = z - k
                yy(zb, c).wait_recv()
                @pl.when(z < Z - 1)
                def _():
                    dn(zb, c).wait_recv()
                    dbuf[zb, rows(c)] = (own(zb, c) + f(abuf[zb, rows(c)])).astype(dbuf.dtype)
                @pl.when(z == Z - 1)
                def _():
                    dbuf[zb, rows(c)] = own(zb, c).astype(dbuf.dtype)
                dn(zb, c).start()
    for c in range(C):
        yy(z, c).wait_recv()
        out_ref[rows(c)] = own(z, c)
        @pl.when(z > 0)
        def _():
            up(z, c).wait_recv()
            out_ref[rows(c)] += f(bbuf[z, rows(c)])
        @pl.when(z < Z - 1)
        def _():
            dn(z, c).wait_recv()
            out_ref[rows(c)] += f(abuf[z, rows(c)])
    for zb in range(Z):
        for c in range(C):
            yy(zb, c).wait_send()
            @pl.when(zb > z)
            def _(): up(zb, c).wait_send()
            @pl.when(zb < z)
            def _(): dn(zb, c).wait_send()

def rs(p, Z, C, cid=2):
    _, R, D = p.shape
    return pl.pallas_call(functools.partial(rs_kernel, Z, C),
        out_shape=jax.ShapeDtypeStruct((R, D), jnp.float32),
        in_specs=[pl.BlockSpec(memory_space=pltpu.VMEM)], out_specs=pl.BlockSpec(memory_space=pltpu.VMEM),
        scratch_shapes=[pltpu.VMEM((Z, R, D), p.dtype)] * 5 + [pltpu.SemaphoreType.DMA((Z, C))] * 6,
        compiler_params=pltpu.CompilerParams(collective_id=cid, has_side_effects=True, vmem_limit_bytes=60 << 20))(p)


def gather_rows(rows, cid):
    full = ag(rows, lax.axis_size("mlp"), 2, cid)
    return full.reshape(-1, rows.shape[1])


def scatter_rows(partial, cid):
    levels = lax.axis_size("mlp")
    return rs(partial.reshape(2 * levels, -1, partial.shape[1]), levels, 2, cid)


def scaled_norm(values, norm_gain):
    return (
        values
        * lax.rsqrt(jnp.mean(values * values, axis=-1, keepdims=True) + norm_epsilon)
        * norm_gain
    )


def rotate(values, cosine_table, sine_table):
    middle = values.shape[-1] // 2
    front_half = values[..., :middle]
    back_half = values[..., middle:]
    return jnp.concatenate(
        [
            front_half * cosine_table - back_half * sine_table,
            back_half * cosine_table + front_half * sine_table,
        ],
        axis=-1,
    )


def rotary_tables(position, head_width):
    middle = head_width // 2
    frequency = jnp.exp(
        -(2.0 * jnp.arange(middle, dtype=jnp.float32) / head_width) * math.log(rope_base)
    )
    angles = position.astype(jnp.float32)[:, None] * frequency[None, :]
    return (jnp.cos(angles), jnp.sin(angles))


def document_layout(lengths, total_rows):
    end_points = jnp.cumsum(lengths)
    row_index = jnp.arange(total_rows, dtype=jnp.int32)
    passed = (row_index[:, None] >= end_points[None, :]).astype(jnp.int32)
    segment = jnp.sum(passed, axis=1)
    offset = jnp.sum(passed * lengths[None, :], axis=1)
    return (segment, row_index - offset)


def attention_classes(item_count, group_cols, query_cols, head_width):
    column = jnp.arange(item_count, dtype=jnp.int32) % group_cols
    return jnp.where(
        column < query_cols,
        0,
        jnp.where(
            column < query_cols + head_width,
            1,
            jnp.where(column < query_cols + 2 * head_width, 2, 3),
        ),
    ).astype(jnp.int32)


def forward_classes(item_count, group_cols):
    column = jnp.arange(item_count, dtype=jnp.int32) % group_cols
    return 4 + (column >= group_cols // 2).astype(jnp.int32)


def output_classes(item_count, group_rows, query_cols):
    row_index = jnp.arange(item_count, dtype=jnp.int32) % group_rows
    return 6 + (row_index >= query_cols).astype(jnp.int32)


def indicator_matrix(class_index):
    return (class_index[:, None] == jnp.arange(8, dtype=jnp.int32)[None, :]).astype(jnp.float32)


def kind_sums(matrix, kind_table, over_axis):
    return jnp.dot(
        jnp.sum(matrix * matrix, axis=over_axis), kind_table, precision=highest_precision
    )


def adam_terms(
    weight, gradient, first_moment, second_moment, correct_one, correct_two, decay_weight
):
    first_new = beta_one * first_moment + (1.0 - beta_one) * gradient
    second_new = beta_two * second_moment + (1.0 - beta_two) * gradient * gradient
    direction = (
        first_new / correct_one / (jnp.sqrt(second_new / correct_two) + adam_epsilon)
        + decay_weight * weight
    )
    return (first_new, second_new, direction)


def swiglu(gate_up_product):
    middle = gate_up_product.shape[-1] // 2
    return jax.nn.silu(gate_up_product[:, :middle]) * gate_up_product[:, middle:]


def contract_first(left, right):
    return lax.dot_general(
        left, right, (((0,), (0,)), ((), ())), preferred_element_type=jnp.float32
    )


def contract_last(left, right):
    return lax.dot_general(
        left, right, (((1,), (1,)), ((), ())), preferred_element_type=jnp.float32
    )


def visibility(segment, begin_row, end_row):
    row_index = jnp.arange(begin_row, end_row, dtype=jnp.int32)
    key_index = jnp.arange(end_row, dtype=jnp.int32)
    same_document = segment[begin_row:end_row, None] == segment[None, :end_row]
    return same_document & (key_index[None, :] <= row_index[:, None])


def block_scores(query_low, key_low, visible, begin_row, end_row, scaling):
    scores = (
        jnp.einsum(
            "qhd,kd->hqk",
            query_low[begin_row:end_row],
            key_low[:end_row],
            preferred_element_type=jnp.float32,
        )
        * scaling
    )
    return jnp.where(visible[None], scores, masked_score)


def shards(
    tokens,
    cotangent,
    attention_in,
    feedforward_in,
    projection_out,
    attention_mean,
    feedforward_mean,
    projection_mean,
    attention_power,
    feedforward_power,
    projection_power,
    gains,
    gain_mean,
    gain_power,
    document_lengths,
    step_count,
):
    own_rows = tokens.shape[0]
    model_width = tokens.shape[1]
    total_rows = own_rows * lax.axis_size(("mlp", "head"))
    head_width = (gains.shape[0] - 2 * model_width) // 2
    attention_cols = attention_in.shape[1]
    query_cols = attention_cols // 2 - head_width
    query_heads = query_cols // head_width
    feed_cols = feedforward_in.shape[1]
    output_rows = projection_out.shape[0]
    gain_one = gains[:model_width]
    gain_two = gains[model_width : 2 * model_width]
    gain_query = gains[2 * model_width : 2 * model_width + head_width]
    gain_key = gains[2 * model_width + head_width :]
    attention_lookup = indicator_matrix(
        attention_classes(attention_cols, attention_cols, query_cols, head_width)
    )
    forward_lookup = indicator_matrix(forward_classes(feed_cols, feed_cols))
    output_lookup = indicator_matrix(output_classes(output_rows, output_rows, query_cols))
    weight_local = (
        kind_sums(attention_in, attention_lookup, 0)
        + kind_sums(feedforward_in, forward_lookup, 0)
        + kind_sums(projection_out, output_lookup, 1)
    )
    attention_reduced, forward_reduced, output_reduced = (
        lax.all_gather(attention_in.astype(jnp.bfloat16), "seq", axis=0, tiled=True),
        lax.all_gather(feedforward_in.astype(jnp.bfloat16), "seq", axis=0, tiled=True),
        lax.all_gather(projection_out.astype(jnp.bfloat16), "seq", axis=1, tiled=True),
    )
    mixer_low = output_reduced[:query_cols]
    down_low = output_reduced[query_cols:]
    segment, position = document_layout(document_lengths[0], total_rows)
    cosine_table, sine_table = rotary_tables(position, head_width)
    inputs = tokens.astype(jnp.float32)
    normed_input, back_one = jax.vjp(scaled_norm, inputs, gain_one)
    normed_rows = gather_rows(normed_input.astype(jnp.bfloat16), 1)
    projected_rows = jnp.dot(normed_rows, attention_reduced, preferred_element_type=jnp.float32)
    query_rows = projected_rows[:, :query_cols].reshape(total_rows, query_heads, head_width)
    keys_raw = projected_rows[:, query_cols : query_cols + head_width]
    values_low = projected_rows[:, query_cols + head_width : query_cols + 2 * head_width].astype(
        jnp.bfloat16
    )
    gate_scores_raw = projected_rows[:, query_cols + 2 * head_width :]

    def prepare(query_in, key_in, query_gain, key_gain):
        query_out = rotate(
            scaled_norm(query_in, query_gain), cosine_table[:, None, :], sine_table[:, None, :]
        )
        key_out = rotate(scaled_norm(key_in, key_gain), cosine_table, sine_table)
        return (query_out, key_out)

    (query_rot, key_rot), back_prepare = jax.vjp(
        prepare, query_rows, keys_raw, gain_query, gain_key
    )
    query_low = query_rot.astype(jnp.bfloat16)
    key_low = key_rot.astype(jnp.bfloat16)
    block_rows = min(512, total_rows)
    block_count = total_rows // block_rows
    scaling = head_width ** (-0.5)
    pieces = []
    log_totals = []
    for block_index in range(block_count):
        begin_row = block_index * block_rows
        end_row = begin_row + block_rows
        visible = visibility(segment, begin_row, end_row)
        scores = block_scores(query_low, key_low, visible, begin_row, end_row, scaling)
        row_max = jnp.max(scores, axis=-1, keepdims=True)
        log_total = row_max + jnp.log(jnp.sum(jnp.exp(scores - row_max), axis=-1, keepdims=True))
        softmax_low = jnp.exp(scores - log_total).astype(jnp.bfloat16)
        pieces.append(
            jnp.einsum(
                "hqk,kd->qhd", softmax_low, values_low[:end_row], preferred_element_type=jnp.float32
            )
        )
        log_totals.append(log_total)
    attended_rows = jnp.concatenate(pieces, axis=0).reshape(total_rows, query_cols)
    gate_sigmoid = jax.nn.sigmoid(gate_scores_raw)
    gated_low = (attended_rows * gate_sigmoid).astype(jnp.bfloat16)
    attention_out = scatter_rows(
        jnp.dot(gated_low, mixer_low, preferred_element_type=jnp.float32).astype(jnp.bfloat16), 2
    )
    middle = inputs + attention_out
    normed_second, back_two = jax.vjp(scaled_norm, middle, gain_two)
    feed_rows = gather_rows(normed_second.astype(jnp.bfloat16), 3)
    gate_up_product = jnp.dot(feed_rows, forward_reduced, preferred_element_type=jnp.float32)
    activated, back_swiglu = jax.vjp(swiglu, gate_up_product)
    activated_low = activated.astype(jnp.bfloat16)
    feed_out = lax.psum_scatter(
        jnp.dot(activated_low, down_low, preferred_element_type=jnp.float32).astype(jnp.bfloat16),
        ("mlp", "head"),
        scatter_dimension=0,
        tiled=True,
    ).astype(jnp.float32)
    block_output = (middle + feed_out).astype(jnp.bfloat16)
    cotangent_rows = lax.all_gather(cotangent, ("mlp", "head"), axis=0, tiled=True)
    delta_activated = contract_last(cotangent_rows, down_low)
    delta_gate_up = back_swiglu(delta_activated)[0].astype(jnp.bfloat16)
    down_gradient = contract_first(activated_low, cotangent_rows)
    feed_gradient = contract_first(feed_rows, delta_gate_up)
    delta_normed_two = scatter_rows(
        contract_last(delta_gate_up, forward_reduced).astype(jnp.bfloat16), 4
    )
    delta_middle_part, delta_gain_two = back_two(delta_normed_two)
    delta_middle = cotangent.astype(jnp.float32) + delta_middle_part
    branch_rows = gather_rows(delta_middle.astype(jnp.bfloat16), 5)
    delta_gated = contract_last(branch_rows, mixer_low)
    mixer_gradient = contract_first(gated_low, branch_rows)
    delta_attended = delta_gated * gate_sigmoid
    delta_logits = delta_gated * attended_rows * gate_sigmoid * (1.0 - gate_sigmoid)
    delta_attended_low = delta_attended.astype(jnp.bfloat16).reshape(
        total_rows, query_heads, head_width
    )
    query_deltas = []
    key_delta = jnp.zeros((total_rows, head_width), jnp.float32)
    value_delta = jnp.zeros((total_rows, head_width), jnp.float32)
    for block_index in range(block_count):
        begin_row = block_index * block_rows
        end_row = begin_row + block_rows
        visible = visibility(segment, begin_row, end_row)
        scores = block_scores(query_low, key_low, visible, begin_row, end_row, scaling)
        softmax_full = jnp.exp(scores - log_totals[block_index])
        softmax_low = softmax_full.astype(jnp.bfloat16)
        delta_rows = delta_attended_low[begin_row:end_row]
        delta_softmax = jnp.einsum(
            "qhd,kd->hqk", delta_rows, values_low[:end_row], preferred_element_type=jnp.float32
        )
        inner_sum = jnp.sum(softmax_full * delta_softmax, axis=-1, keepdims=True)
        delta_scores = (softmax_full * (delta_softmax - inner_sum)).astype(jnp.bfloat16)
        query_deltas.append(
            jnp.einsum(
                "hqk,kd->qhd", delta_scores, key_low[:end_row], preferred_element_type=jnp.float32
            )
            * scaling
        )
        key_delta = key_delta.at[:end_row].add(
            jnp.einsum(
                "hqk,qhd->kd",
                delta_scores,
                query_low[begin_row:end_row],
                preferred_element_type=jnp.float32,
            )
            * scaling
        )
        value_delta = value_delta.at[:end_row].add(
            jnp.einsum("hqk,qhd->kd", softmax_low, delta_rows, preferred_element_type=jnp.float32)
        )
    query_delta = jnp.concatenate(query_deltas, axis=0)
    query_back, key_back, delta_gain_query, delta_gain_key = back_prepare((query_delta, key_delta))
    delta_projected = jnp.concatenate(
        [query_back.reshape(total_rows, query_cols), key_back, value_delta, delta_logits], axis=1
    ).astype(jnp.bfloat16)
    delta_normed = scatter_rows(
        contract_last(delta_projected, attention_reduced).astype(jnp.bfloat16), 6
    )
    delta_input_part, delta_gain_one = back_one(delta_normed)
    input_gradient = delta_middle + delta_input_part
    attention_gradient = contract_first(normed_rows, delta_projected)
    output_gradient = jnp.concatenate([mixer_gradient, down_gradient], axis=0)
    attention_total, feed_total, output_total = (
        lax.psum_scatter(
            attention_gradient.astype(jnp.bfloat16), "seq", scatter_dimension=0, tiled=True
        ).astype(jnp.float32),
        lax.psum_scatter(
            feed_gradient.astype(jnp.bfloat16), "seq", scatter_dimension=0, tiled=True
        ).astype(jnp.float32),
        lax.psum_scatter(
            output_gradient.astype(jnp.bfloat16), "seq", scatter_dimension=1, tiled=True
        ).astype(jnp.float32),
    )
    steps_done = step_count[0].astype(jnp.float32)
    correct_one = 1.0 - jnp.power(beta_one, steps_done)
    correct_two = 1.0 - jnp.power(beta_two, steps_done)
    mean_attention, power_attention, move_attention = adam_terms(
        attention_in,
        attention_total,
        attention_mean,
        attention_power,
        correct_one,
        correct_two,
        decay_rate,
    )
    mean_feedforward, power_feedforward, move_feed = adam_terms(
        feedforward_in,
        feed_total,
        feedforward_mean,
        feedforward_power,
        correct_one,
        correct_two,
        decay_rate,
    )
    mean_projection, power_projection, move_output = adam_terms(
        projection_out,
        output_total,
        projection_mean,
        projection_power,
        correct_one,
        correct_two,
        decay_rate,
    )
    update_local = (
        kind_sums(move_attention, attention_lookup, 0)
        + kind_sums(move_feed, forward_lookup, 0)
        + kind_sums(move_output, output_lookup, 1)
    )
    gain_local = jnp.concatenate([delta_gain_one, delta_gain_two, delta_gain_query, delta_gain_key])
    norm_local = jnp.concatenate([weight_local, update_local])
    gain_total, norm_total = lax.psum((gain_local, norm_local), ("seq", "mlp", "head"))
    weight_squares = norm_total[:8]
    update_squares = norm_total[8:]
    trust_ratio = jnp.sqrt(weight_squares) / jnp.sqrt(update_squares)
    attention_master = (
        attention_in
        - learn_rate
        * jnp.dot(attention_lookup, trust_ratio, precision=highest_precision)[None, :]
        * move_attention
    )
    feedforward_master = (
        feedforward_in
        - learn_rate
        * jnp.dot(forward_lookup, trust_ratio, precision=highest_precision)[None, :]
        * move_feed
    )
    projection_master = (
        projection_out
        - learn_rate
        * jnp.dot(output_lookup, trust_ratio, precision=highest_precision)[:, None]
        * move_output
    )
    mean_gains, power_gains, move_gains = adam_terms(
        gains, gain_total, gain_mean, gain_power, correct_one, correct_two, 0.0
    )
    gains_next = gains - learn_rate * move_gains
    matrix_norms = jnp.stack([jnp.sqrt(weight_squares), jnp.sqrt(update_squares)])
    return (
        block_output,
        input_gradient,
        attention_master,
        feedforward_master,
        projection_master,
        mean_attention,
        mean_feedforward,
        mean_projection,
        power_attention,
        power_feedforward,
        power_projection,
        attention_master.astype(jnp.bfloat16),
        feedforward_master.astype(jnp.bfloat16),
        projection_master.astype(jnp.bfloat16),
        gains_next,
        mean_gains,
        power_gains,
        matrix_norms,
    )


def solution(mesh):
    placed = (
        P(("seq", "mlp", "head"), None),
        P(("seq", "mlp", "head"), None),
        P("seq", ("mlp", "head")),
        P("seq", ("mlp", "head")),
        P(("mlp", "head"), "seq"),
        P("seq", ("mlp", "head")),
        P("seq", ("mlp", "head")),
        P(("mlp", "head"), "seq"),
        P("seq", ("mlp", "head")),
        P("seq", ("mlp", "head")),
        P(("mlp", "head"), "seq"),
        P(),
        P(),
        P(),
        P("seq", None),
        P(),
    )
    return jax.shard_map(
        shards,
        mesh=mesh,
        in_specs=placed,
        out_specs=(
            P(("seq", "mlp", "head"), None),
            P(("seq", "mlp", "head"), None),
            P("seq", ("mlp", "head")),
            P("seq", ("mlp", "head")),
            P(("mlp", "head"), "seq"),
            P("seq", ("mlp", "head")),
            P("seq", ("mlp", "head")),
            P(("mlp", "head"), "seq"),
            P("seq", ("mlp", "head")),
            P("seq", ("mlp", "head")),
            P(("mlp", "head"), "seq"),
            P("seq", ("mlp", "head")),
            P("seq", ("mlp", "head")),
            P(("mlp", "head"), "seq"),
            P(),
            P(),
            P(),
            P(),
        ),
        check_vma=False,
    )
```

```python
import functools
import math

import jax
import jax.numpy as jnp
from jax import lax
from jax.experimental import pallas as pl
from jax.experimental.pallas import tpu as pltpu
from jax.sharding import PartitionSpec as P

norm_epsilon = 1e-06
rope_base = 1000000.0
beta_one = 0.9
beta_two = 0.999
adam_epsilon = 1e-08
decay_rate = 0.01
learn_rate = 0.3
masked_score = -1e30
highest_precision = lax.Precision.HIGHEST
MESH = pl.DeviceIdType.MESH


def remote(src, dst, ssem, rsem, dev):
    return pltpu.make_async_remote_copy(src_ref=src, dst_ref=dst, send_sem=ssem, recv_sem=rsem, device_id=dev, device_id_type=MESH)

def enter(Z, z, y):
    bar = pltpu.get_barrier_semaphore()
    pl.semaphore_signal(bar, inc=1, device_id={"head": 1 - y}, device_id_type=MESH)
    @pl.when(z > 0)
    def _():
        pl.semaphore_signal(bar, inc=1, device_id={"mlp": z - 1}, device_id_type=MESH)
    @pl.when(z < Z - 1)
    def _():
        pl.semaphore_signal(bar, inc=1, device_id={"mlp": z + 1}, device_id_type=MESH)
    inner = (z > 0) & (z < Z - 1)
    @pl.when(inner)
    def _(): pl.semaphore_wait(bar, 3)
    @pl.when(jnp.logical_not(inner))
    def _(): pl.semaphore_wait(bar, 2)

def ag_kernel(Z, C, x_ref, out_ref, usem, dsem, ysem, rsem):
    z = lax.axis_index("mlp"); y = lax.axis_index("head")
    R = x_ref.shape[0]; r = R // C
    enter(Z, z, y)
    own = z * 2 + y
    def cp(src, b, c, sem, dev):
        return remote(src, out_ref.at[b, pl.ds(c * r, r)], sem, rsem.at[b, c], dev)
    def blk(b, c): return out_ref.at[b, pl.ds(c * r, r)]
    def up(src, b, zb, c): return cp(src, b, c, usem.at[zb, c], {"mlp": z + 1})
    def dn(src, b, zb, c): return cp(src, b, c, dsem.at[zb, c], {"mlp": z - 1})
    def yy(src, b, zb, c): return cp(src, b, c, ysem.at[zb, c], {"head": 1 - y})
    for c in range(C):
        s = x_ref.at[pl.ds(c * r, r)]
        @pl.when(z < Z - 1)
        def _(): up(s, own, z, c).start()
        @pl.when(z > 0)
        def _(): dn(s, own, z, c).start()
        yy(s, own, z, c).start()
    out_ref[own] = x_ref[...]
    for k in range(1, Z):
        for c in range(C):
            @pl.when(z - k >= 0)
            def _():
                zb = z - k; b = zb * 2 + y
                yy(blk(b, c), b, zb, c).wait_recv()
                @pl.when(z < Z - 1)
                def _(): up(blk(b, c), b, zb, c).start()
                yy(blk(b, c), b, zb, c).start()
            @pl.when(z + k <= Z - 1)
            def _():
                zb = z + k; b = zb * 2 + y
                yy(blk(b, c), b, zb, c).wait_recv()
                @pl.when(z > 0)
                def _(): dn(blk(b, c), b, zb, c).start()
                yy(blk(b, c), b, zb, c).start()
    for zb in range(Z):
        for c in range(C):
            b = zb * 2 + (1 - y)
            yy(blk(b, c), b, zb, c).wait_recv()
    for zb in range(Z):
        for c in range(C):
            b = zb * 2 + y
            yy(blk(b, c), b, zb, c).wait_send()
            @pl.when((z < Z - 1) & (zb <= z))
            def _(): up(blk(b, c), b, zb, c).wait_send()
            @pl.when((z > 0) & (zb >= z))
            def _(): dn(blk(b, c), b, zb, c).wait_send()

def ag(x, Z, C, cid=1):
    R, D = x.shape
    return pl.pallas_call(functools.partial(ag_kernel, Z, C),
        out_shape=jax.ShapeDtypeStruct((2 * Z, R, D), x.dtype),
        in_specs=[pl.BlockSpec(memory_space=pltpu.VMEM)], out_specs=pl.BlockSpec(memory_space=pltpu.VMEM),
        scratch_shapes=[pltpu.SemaphoreType.DMA((Z, C))] * 3 + [pltpu.SemaphoreType.DMA((2 * Z, C))],
        compiler_params=pltpu.CompilerParams(collective_id=cid, has_side_effects=True, vmem_limit_bytes=60 << 20))(x)

def rs_kernel(Z, C, p_ref, out_ref, ybuf, bbuf, abuf, ubuf, dbuf, ysem, usem, dsem, yr, br, ar):
    z = lax.axis_index("mlp"); y = lax.axis_index("head")
    R, D = out_ref.shape; r = R // C
    enter(Z, z, y)
    def rows(c): return pl.ds(c * r, r)
    def yy(zb, c): return remote(p_ref.at[zb * 2 + 1 - y, rows(c)], ybuf.at[zb, rows(c)], ysem.at[zb, c], yr.at[zb, c], {"head": 1 - y})
    def up(zb, c): return remote(ubuf.at[zb, rows(c)], bbuf.at[zb, rows(c)], usem.at[zb, c], br.at[zb, c], {"mlp": z + 1})
    def dn(zb, c): return remote(dbuf.at[zb, rows(c)], abuf.at[zb, rows(c)], dsem.at[zb, c], ar.at[zb, c], {"mlp": z - 1})
    for k in range(Z - 1, -1, -1):
        for c in range(C):
            @pl.when(z + k <= Z - 1)
            def _(): yy(z + k, c).start()
            if k:
                @pl.when(z - k >= 0)
                def _(): yy(z - k, c).start()
    f = lambda v: v.astype(jnp.float32)
    def own(zb, c): return f(p_ref[zb * 2 + y, rows(c)]) + f(ybuf[zb, rows(c)])
    for k in range(Z - 1, 0, -1):
        for c in range(C):
            @pl.when(z + k <= Z - 1)
            def _():
                zb = z + k
                yy(zb, c).wait_recv()
                @pl.when(z > 0)
                def _():
                    up(zb, c).wait_recv()
                    ubuf[zb, rows(c)] = (own(zb, c) + f(bbuf[zb, rows(c)])).astype(ubuf.dtype)
                @pl.when(z == 0)
                def _():
                    ubuf[zb, rows(c)] = own(zb, c).astype(ubuf.dtype)
                up(zb, c).start()
            @pl.when(z - k >= 0)
            def _():
                zb = z - k
                yy(zb, c).wait_recv()
                @pl.when(z < Z - 1)
                def _():
                    dn(zb, c).wait_recv()
                    dbuf[zb, rows(c)] = (own(zb, c) + f(abuf[zb, rows(c)])).astype(dbuf.dtype)
                @pl.when(z == Z - 1)
                def _():
                    dbuf[zb, rows(c)] = own(zb, c).astype(dbuf.dtype)
                dn(zb, c).start()
    for c in range(C):
        yy(z, c).wait_recv()
        out_ref[rows(c)] = own(z, c)
        @pl.when(z > 0)
        def _():
            up(z, c).wait_recv()
            out_ref[rows(c)] += f(bbuf[z, rows(c)])
        @pl.when(z < Z - 1)
        def _():
            dn(z, c).wait_recv()
            out_ref[rows(c)] += f(abuf[z, rows(c)])
    for zb in range(Z):
        for c in range(C):
            yy(zb, c).wait_send()
            @pl.when(zb > z)
            def _(): up(zb, c).wait_send()
            @pl.when(zb < z)
            def _(): dn(zb, c).wait_send()

def rs(p, Z, C, cid=2):
    _, R, D = p.shape
    return pl.pallas_call(functools.partial(rs_kernel, Z, C),
        out_shape=jax.ShapeDtypeStruct((R, D), jnp.float32),
        in_specs=[pl.BlockSpec(memory_space=pltpu.VMEM)], out_specs=pl.BlockSpec(memory_space=pltpu.VMEM),
        scratch_shapes=[pltpu.VMEM((Z, R, D), p.dtype)] * 5 + [pltpu.SemaphoreType.DMA((Z, C))] * 6,
        compiler_params=pltpu.CompilerParams(collective_id=cid, has_side_effects=True, vmem_limit_bytes=60 << 20))(p)


def total_kernel(axes, x_ref, out_ref, *scratch):
    count = len(axes)
    slots, sums, send_sems, recv_sems = (scratch[i * count : (i + 1) * count] for i in range(4))
    barrier = pltpu.get_barrier_semaphore()
    for name, size in axes:
        me = lax.axis_index(name)
        for step in range(1, size):
            pl.semaphore_signal(
                barrier, inc=1, device_id={name: lax.rem(me + step, size)}, device_id_type=MESH
            )
    pl.semaphore_wait(barrier, sum(size - 1 for _, size in axes))
    current = x_ref
    for index, (name, size) in enumerate(axes):
        me = lax.axis_index(name)

        def copy(step):
            return remote(
                current,
                slots[index].at[me],
                send_sems[index].at[step],
                recv_sems[index].at[me],
                {name: lax.rem(me + step, size)},
            )

        def arrival(step):
            source = lax.rem(me + size - step, size)
            return remote(
                current,
                slots[index].at[source],
                send_sems[index].at[step],
                recv_sems[index].at[source],
                {name: lax.rem(me + step, size)},
            )

        for step in range(1, size):
            copy(step).start()
        slots[index][me] = current[...]
        for step in range(1, size):
            arrival(step).wait_recv()
        for step in range(1, size):
            copy(step).wait_send()
        total = slots[index][0]
        for slot in range(1, size):
            total = total + slots[index][slot]
        if index == count - 1:
            out_ref[...] = total
        else:
            sums[index][...] = total
            current = sums[index]


def total_over(values, axes, cid):
    shape = values.shape
    return pl.pallas_call(
        functools.partial(total_kernel, axes),
        out_shape=jax.ShapeDtypeStruct(shape, values.dtype),
        in_specs=[pl.BlockSpec(memory_space=pltpu.VMEM)],
        out_specs=pl.BlockSpec(memory_space=pltpu.VMEM),
        scratch_shapes=[pltpu.VMEM((size, *shape), values.dtype) for _, size in axes]
        + [pltpu.VMEM(shape, values.dtype) for _ in axes]
        + [pltpu.SemaphoreType.DMA((size,)) for _, size in axes] * 2,
        compiler_params=pltpu.CompilerParams(collective_id=cid, has_side_effects=True),
    )(values)


def gather_rows(rows, cid):
    full = ag(rows, lax.axis_size("mlp"), 2, cid)
    return full.reshape(-1, rows.shape[1])


def scatter_rows(partial, cid):
    levels = lax.axis_size("mlp")
    return rs(partial.reshape(2 * levels, -1, partial.shape[1]), levels, 2, cid)


def scaled_norm(values, norm_gain):
    return (
        values
        * lax.rsqrt(jnp.mean(values * values, axis=-1, keepdims=True) + norm_epsilon)
        * norm_gain
    )


def rotate(values, cosine_table, sine_table):
    middle = values.shape[-1] // 2
    front_half = values[..., :middle]
    back_half = values[..., middle:]
    return jnp.concatenate(
        [
            front_half * cosine_table - back_half * sine_table,
            back_half * cosine_table + front_half * sine_table,
        ],
        axis=-1,
    )


def rotary_tables(position, head_width):
    middle = head_width // 2
    frequency = jnp.exp(
        -(2.0 * jnp.arange(middle, dtype=jnp.float32) / head_width) * math.log(rope_base)
    )
    angles = position.astype(jnp.float32)[:, None] * frequency[None, :]
    return (jnp.cos(angles), jnp.sin(angles))


def document_layout(lengths, total_rows):
    end_points = jnp.cumsum(lengths)
    row_index = jnp.arange(total_rows, dtype=jnp.int32)
    passed = (row_index[:, None] >= end_points[None, :]).astype(jnp.int32)
    segment = jnp.sum(passed, axis=1)
    offset = jnp.sum(passed * lengths[None, :], axis=1)
    return (segment, row_index - offset)


def attention_classes(item_count, group_cols, query_cols, head_width):
    column = jnp.arange(item_count, dtype=jnp.int32) % group_cols
    return jnp.where(
        column < query_cols,
        0,
        jnp.where(
            column < query_cols + head_width,
            1,
            jnp.where(column < query_cols + 2 * head_width, 2, 3),
        ),
    ).astype(jnp.int32)


def forward_classes(item_count, group_cols):
    column = jnp.arange(item_count, dtype=jnp.int32) % group_cols
    return 4 + (column >= group_cols // 2).astype(jnp.int32)


def output_classes(item_count, group_rows, query_cols):
    row_index = jnp.arange(item_count, dtype=jnp.int32) % group_rows
    return 6 + (row_index >= query_cols).astype(jnp.int32)


def indicator_matrix(class_index):
    return (class_index[:, None] == jnp.arange(8, dtype=jnp.int32)[None, :]).astype(jnp.float32)


def kind_sums(matrix, kind_table, over_axis):
    return jnp.dot(
        jnp.sum(matrix * matrix, axis=over_axis), kind_table, precision=highest_precision
    )


def adam_terms(
    weight, gradient, first_moment, second_moment, correct_one, correct_two, decay_weight
):
    first_new = beta_one * first_moment + (1.0 - beta_one) * gradient
    second_new = beta_two * second_moment + (1.0 - beta_two) * gradient * gradient
    direction = (
        first_new / correct_one / (jnp.sqrt(second_new / correct_two) + adam_epsilon)
        + decay_weight * weight
    )
    return (first_new, second_new, direction)


def swiglu(gate_up_product):
    middle = gate_up_product.shape[-1] // 2
    return jax.nn.silu(gate_up_product[:, :middle]) * gate_up_product[:, middle:]


def contract_first(left, right):
    return lax.dot_general(
        left, right, (((0,), (0,)), ((), ())), preferred_element_type=jnp.float32
    )


def contract_last(left, right):
    return lax.dot_general(
        left, right, (((1,), (1,)), ((), ())), preferred_element_type=jnp.float32
    )


def visibility(segment, begin_row, end_row):
    row_index = jnp.arange(begin_row, end_row, dtype=jnp.int32)
    key_index = jnp.arange(end_row, dtype=jnp.int32)
    same_document = segment[begin_row:end_row, None] == segment[None, :end_row]
    return same_document & (key_index[None, :] <= row_index[:, None])


def block_scores(query_low, key_low, visible, begin_row, end_row, scaling):
    scores = (
        jnp.einsum(
            "qhd,kd->hqk",
            query_low[begin_row:end_row],
            key_low[:end_row],
            preferred_element_type=jnp.float32,
        )
        * scaling
    )
    return jnp.where(visible[None], scores, masked_score)


def shards(
    tokens,
    cotangent,
    attention_in,
    feedforward_in,
    projection_out,
    attention_mean,
    feedforward_mean,
    projection_mean,
    attention_power,
    feedforward_power,
    projection_power,
    gains,
    gain_mean,
    gain_power,
    document_lengths,
    step_count,
):
    own_rows = tokens.shape[0]
    model_width = tokens.shape[1]
    total_rows = own_rows * lax.axis_size(("mlp", "head"))
    head_width = (gains.shape[0] - 2 * model_width) // 2
    attention_cols = attention_in.shape[1]
    query_cols = attention_cols // 2 - head_width
    query_heads = query_cols // head_width
    feed_cols = feedforward_in.shape[1]
    output_rows = projection_out.shape[0]
    gain_one = gains[:model_width]
    gain_two = gains[model_width : 2 * model_width]
    gain_query = gains[2 * model_width : 2 * model_width + head_width]
    gain_key = gains[2 * model_width + head_width :]
    attention_lookup = indicator_matrix(
        attention_classes(attention_cols, attention_cols, query_cols, head_width)
    )
    forward_lookup = indicator_matrix(forward_classes(feed_cols, feed_cols))
    output_lookup = indicator_matrix(output_classes(output_rows, output_rows, query_cols))
    weight_local = (
        kind_sums(attention_in, attention_lookup, 0)
        + kind_sums(feedforward_in, forward_lookup, 0)
        + kind_sums(projection_out, output_lookup, 1)
    )
    attention_reduced, forward_reduced, output_reduced = (
        lax.all_gather(attention_in.astype(jnp.bfloat16), "seq", axis=0, tiled=True),
        lax.all_gather(feedforward_in.astype(jnp.bfloat16), "seq", axis=0, tiled=True),
        lax.all_gather(projection_out.astype(jnp.bfloat16), "seq", axis=1, tiled=True),
    )
    mixer_low = output_reduced[:query_cols]
    down_low = output_reduced[query_cols:]
    segment, position = document_layout(document_lengths[0], total_rows)
    cosine_table, sine_table = rotary_tables(position, head_width)
    inputs = tokens.astype(jnp.float32)
    normed_input, back_one = jax.vjp(scaled_norm, inputs, gain_one)
    normed_rows = gather_rows(normed_input.astype(jnp.bfloat16), 1)
    projected_rows = jnp.dot(normed_rows, attention_reduced, preferred_element_type=jnp.float32)
    query_rows = projected_rows[:, :query_cols].reshape(total_rows, query_heads, head_width)
    keys_raw = projected_rows[:, query_cols : query_cols + head_width]
    values_low = projected_rows[:, query_cols + head_width : query_cols + 2 * head_width].astype(
        jnp.bfloat16
    )
    gate_scores_raw = projected_rows[:, query_cols + 2 * head_width :]

    def prepare(query_in, key_in, query_gain, key_gain):
        query_out = rotate(
            scaled_norm(query_in, query_gain), cosine_table[:, None, :], sine_table[:, None, :]
        )
        key_out = rotate(scaled_norm(key_in, key_gain), cosine_table, sine_table)
        return (query_out, key_out)

    (query_rot, key_rot), back_prepare = jax.vjp(
        prepare, query_rows, keys_raw, gain_query, gain_key
    )
    query_low = query_rot.astype(jnp.bfloat16)
    key_low = key_rot.astype(jnp.bfloat16)
    block_rows = min(512, total_rows)
    block_count = total_rows // block_rows
    scaling = head_width ** (-0.5)
    pieces = []
    log_totals = []
    for block_index in range(block_count):
        begin_row = block_index * block_rows
        end_row = begin_row + block_rows
        visible = visibility(segment, begin_row, end_row)
        scores = block_scores(query_low, key_low, visible, begin_row, end_row, scaling)
        row_max = jnp.max(scores, axis=-1, keepdims=True)
        log_total = row_max + jnp.log(jnp.sum(jnp.exp(scores - row_max), axis=-1, keepdims=True))
        softmax_low = jnp.exp(scores - log_total).astype(jnp.bfloat16)
        pieces.append(
            jnp.einsum(
                "hqk,kd->qhd", softmax_low, values_low[:end_row], preferred_element_type=jnp.float32
            )
        )
        log_totals.append(log_total)
    attended_rows = jnp.concatenate(pieces, axis=0).reshape(total_rows, query_cols)
    gate_sigmoid = jax.nn.sigmoid(gate_scores_raw)
    gated_low = (attended_rows * gate_sigmoid).astype(jnp.bfloat16)
    attention_out = scatter_rows(
        jnp.dot(gated_low, mixer_low, preferred_element_type=jnp.float32).astype(jnp.bfloat16), 2
    )
    middle = inputs + attention_out
    normed_second, back_two = jax.vjp(scaled_norm, middle, gain_two)
    feed_rows = gather_rows(normed_second.astype(jnp.bfloat16), 3)
    gate_up_product = jnp.dot(feed_rows, forward_reduced, preferred_element_type=jnp.float32)
    activated, back_swiglu = jax.vjp(swiglu, gate_up_product)
    activated_low = activated.astype(jnp.bfloat16)
    cotangent_rows = lax.all_gather(cotangent, ("mlp", "head"), axis=0, tiled=True)
    delta_activated = contract_last(cotangent_rows, down_low)
    delta_gate_up = back_swiglu(delta_activated)[0].astype(jnp.bfloat16)
    down_gradient, feed_gradient, feed_delta_partial = lax.optimization_barrier(
        (
            contract_first(activated_low, cotangent_rows).astype(jnp.bfloat16),
            contract_first(feed_rows, delta_gate_up).astype(jnp.bfloat16),
            contract_last(delta_gate_up, forward_reduced).astype(jnp.bfloat16),
        )
    )
    feed_total = lax.psum_scatter(
        feed_gradient, "seq", scatter_dimension=0, tiled=True
    ).astype(jnp.float32)
    down_total = lax.psum_scatter(
        down_gradient, "seq", scatter_dimension=1, tiled=True
    ).astype(jnp.float32)
    delta_normed_two = scatter_rows(feed_delta_partial, 4)
    delta_middle_part, delta_gain_two = back_two(delta_normed_two)
    delta_middle = cotangent.astype(jnp.float32) + delta_middle_part
    branch_rows, feed_out_partial = lax.optimization_barrier(
        (
            gather_rows(delta_middle.astype(jnp.bfloat16), 5),
            jnp.dot(activated_low, down_low, preferred_element_type=jnp.float32).astype(
                jnp.bfloat16
            ),
        )
    )
    feed_out = lax.psum_scatter(
        feed_out_partial, ("mlp", "head"), scatter_dimension=0, tiled=True
    ).astype(jnp.float32)
    block_output = (middle + feed_out).astype(jnp.bfloat16)
    delta_gated = contract_last(branch_rows, mixer_low)
    mixer_total = lax.psum_scatter(
        contract_first(gated_low, branch_rows).astype(jnp.bfloat16),
        "seq",
        scatter_dimension=1,
        tiled=True,
    ).astype(jnp.float32)
    delta_attended = delta_gated * gate_sigmoid
    delta_logits = delta_gated * attended_rows * gate_sigmoid * (1.0 - gate_sigmoid)
    delta_attended_low = delta_attended.astype(jnp.bfloat16).reshape(
        total_rows, query_heads, head_width
    )
    query_deltas = []
    key_delta = jnp.zeros((total_rows, head_width), jnp.float32)
    value_delta = jnp.zeros((total_rows, head_width), jnp.float32)
    for block_index in range(block_count):
        begin_row = block_index * block_rows
        end_row = begin_row + block_rows
        visible = visibility(segment, begin_row, end_row)
        scores = block_scores(query_low, key_low, visible, begin_row, end_row, scaling)
        softmax_full = jnp.exp(scores - log_totals[block_index])
        softmax_low = softmax_full.astype(jnp.bfloat16)
        delta_rows = delta_attended_low[begin_row:end_row]
        delta_softmax = jnp.einsum(
            "qhd,kd->hqk", delta_rows, values_low[:end_row], preferred_element_type=jnp.float32
        )
        inner_sum = jnp.sum(softmax_full * delta_softmax, axis=-1, keepdims=True)
        delta_scores = (softmax_full * (delta_softmax - inner_sum)).astype(jnp.bfloat16)
        query_deltas.append(
            jnp.einsum(
                "hqk,kd->qhd", delta_scores, key_low[:end_row], preferred_element_type=jnp.float32
            )
            * scaling
        )
        key_delta = key_delta.at[:end_row].add(
            jnp.einsum(
                "hqk,qhd->kd",
                delta_scores,
                query_low[begin_row:end_row],
                preferred_element_type=jnp.float32,
            )
            * scaling
        )
        value_delta = value_delta.at[:end_row].add(
            jnp.einsum("hqk,qhd->kd", softmax_low, delta_rows, preferred_element_type=jnp.float32)
        )
    query_delta = jnp.concatenate(query_deltas, axis=0)
    query_back, key_back, delta_gain_query, delta_gain_key = back_prepare((query_delta, key_delta))
    delta_projected = jnp.concatenate(
        [query_back.reshape(total_rows, query_cols), key_back, value_delta, delta_logits], axis=1
    ).astype(jnp.bfloat16)
    attention_gradient, delta_partial = lax.optimization_barrier(
        (
            contract_first(normed_rows, delta_projected).astype(jnp.bfloat16),
            contract_last(delta_projected, attention_reduced).astype(jnp.bfloat16),
        )
    )
    attention_total = lax.psum_scatter(
        attention_gradient, "seq", scatter_dimension=0, tiled=True
    ).astype(jnp.float32)
    delta_normed = scatter_rows(delta_partial, 6)
    delta_input_part, delta_gain_one = back_one(delta_normed)
    input_gradient = delta_middle + delta_input_part
    output_total = jnp.concatenate([mixer_total, down_total], axis=0)
    steps_done = step_count[0].astype(jnp.float32)
    correct_one = 1.0 - jnp.power(beta_one, steps_done)
    correct_two = 1.0 - jnp.power(beta_two, steps_done)
    mean_attention, power_attention, move_attention = adam_terms(
        attention_in,
        attention_total,
        attention_mean,
        attention_power,
        correct_one,
        correct_two,
        decay_rate,
    )
    mean_feedforward, power_feedforward, move_feed = adam_terms(
        feedforward_in,
        feed_total,
        feedforward_mean,
        feedforward_power,
        correct_one,
        correct_two,
        decay_rate,
    )
    mean_projection, power_projection, move_output = adam_terms(
        projection_out,
        output_total,
        projection_mean,
        projection_power,
        correct_one,
        correct_two,
        decay_rate,
    )
    update_local = (
        kind_sums(move_attention, attention_lookup, 0)
        + kind_sums(move_feed, forward_lookup, 0)
        + kind_sums(move_output, output_lookup, 1)
    )
    gain_local = jnp.concatenate([delta_gain_one, delta_gain_two, delta_gain_query, delta_gain_key])
    norm_local = jnp.concatenate([weight_local, update_local])
    packed = jnp.concatenate([gain_local, norm_local])
    packed_rows = -(-packed.shape[0] // 1024) * 8
    packed_total = total_over(
        jnp.pad(packed, (0, packed_rows * 128 - packed.shape[0])).reshape(packed_rows, 128),
        tuple((name, lax.axis_size(name)) for name in ("seq", "mlp", "head")),
        7,
    ).reshape(-1)
    gain_total = packed_total[: gain_local.shape[0]]
    norm_total = packed_total[gain_local.shape[0] : packed.shape[0]]
    weight_squares = norm_total[:8]
    update_squares = norm_total[8:]
    trust_ratio = jnp.sqrt(weight_squares) / jnp.sqrt(update_squares)
    attention_master = (
        attention_in
        - learn_rate
        * jnp.dot(attention_lookup, trust_ratio, precision=highest_precision)[None, :]
        * move_attention
    )
    feedforward_master = (
        feedforward_in
        - learn_rate
        * jnp.dot(forward_lookup, trust_ratio, precision=highest_precision)[None, :]
        * move_feed
    )
    projection_master = (
        projection_out
        - learn_rate
        * jnp.dot(output_lookup, trust_ratio, precision=highest_precision)[:, None]
        * move_output
    )
    mean_gains, power_gains, move_gains = adam_terms(
        gains, gain_total, gain_mean, gain_power, correct_one, correct_two, 0.0
    )
    gains_next = gains - learn_rate * move_gains
    matrix_norms = jnp.stack([jnp.sqrt(weight_squares), jnp.sqrt(update_squares)])
    return (
        block_output,
        input_gradient,
        attention_master,
        feedforward_master,
        projection_master,
        mean_attention,
        mean_feedforward,
        mean_projection,
        power_attention,
        power_feedforward,
        power_projection,
        attention_master.astype(jnp.bfloat16),
        feedforward_master.astype(jnp.bfloat16),
        projection_master.astype(jnp.bfloat16),
        gains_next,
        mean_gains,
        power_gains,
        matrix_norms,
    )


def solution(mesh):
    placed = (
        P(("seq", "mlp", "head"), None),
        P(("seq", "mlp", "head"), None),
        P("seq", ("mlp", "head")),
        P("seq", ("mlp", "head")),
        P(("mlp", "head"), "seq"),
        P("seq", ("mlp", "head")),
        P("seq", ("mlp", "head")),
        P(("mlp", "head"), "seq"),
        P("seq", ("mlp", "head")),
        P("seq", ("mlp", "head")),
        P(("mlp", "head"), "seq"),
        P(),
        P(),
        P(),
        P("seq", None),
        P(),
    )
    return jax.shard_map(
        shards,
        mesh=mesh,
        in_specs=placed,
        out_specs=(
            P(("seq", "mlp", "head"), None),
            P(("seq", "mlp", "head"), None),
            P("seq", ("mlp", "head")),
            P("seq", ("mlp", "head")),
            P(("mlp", "head"), "seq"),
            P("seq", ("mlp", "head")),
            P("seq", ("mlp", "head")),
            P(("mlp", "head"), "seq"),
            P("seq", ("mlp", "head")),
            P("seq", ("mlp", "head")),
            P(("mlp", "head"), "seq"),
            P("seq", ("mlp", "head")),
            P("seq", ("mlp", "head")),
            P(("mlp", "head"), "seq"),
            P(),
            P(),
            P(),
            P(),
        ),
        check_vma=False,
    )
```

```python
import functools
import math

import jax
import jax.numpy as jnp
from jax import lax
from jax.experimental import pallas as pl
from jax.experimental.pallas import tpu as pltpu
from jax.sharding import PartitionSpec as P


norm_epsilon = 1e-06
rope_base = 1000000.0
beta_one = 0.9
beta_two = 0.999
adam_epsilon = 1e-08
decay_rate = 0.01
learn_rate = 0.3
masked_score = -1e30
highest_precision = lax.Precision.HIGHEST
MESH = pl.DeviceIdType.MESH


def remote(src, dst, ssem, rsem, dev):
    return pltpu.make_async_remote_copy(src_ref=src, dst_ref=dst, send_sem=ssem, recv_sem=rsem, device_id=dev, device_id_type=MESH)


def enter(Z, z, y):
    bar = pltpu.get_barrier_semaphore()
    pl.semaphore_signal(bar, inc=1, device_id={"head": 1 - y}, device_id_type=MESH)
    @pl.when(z > 0)
    def _():
        pl.semaphore_signal(bar, inc=1, device_id={"mlp": z - 1}, device_id_type=MESH)
    @pl.when(z < Z - 1)
    def _():
        pl.semaphore_signal(bar, inc=1, device_id={"mlp": z + 1}, device_id_type=MESH)
    inner = (z > 0) & (z < Z - 1)
    @pl.when(inner)
    def _(): pl.semaphore_wait(bar, 3)
    @pl.when(jnp.logical_not(inner))
    def _(): pl.semaphore_wait(bar, 2)


def ag_kernel(Z, C, x_ref, out_ref, usem, dsem, ysem, rsem):
    z = lax.axis_index("mlp"); y = lax.axis_index("head")
    R = x_ref.shape[0]; r = R // C
    enter(Z, z, y)
    own = z * 2 + y
    def cp(src, b, c, sem, dev):
        return remote(src, out_ref.at[b, pl.ds(c * r, r)], sem, rsem.at[b, c], dev)
    def blk(b, c): return out_ref.at[b, pl.ds(c * r, r)]
    def up(src, b, zb, c): return cp(src, b, c, usem.at[zb, c], {"mlp": z + 1})
    def dn(src, b, zb, c): return cp(src, b, c, dsem.at[zb, c], {"mlp": z - 1})
    def yy(src, b, zb, c): return cp(src, b, c, ysem.at[zb, c], {"head": 1 - y})
    for c in range(C):
        s = x_ref.at[pl.ds(c * r, r)]
        @pl.when(z < Z - 1)
        def _(): up(s, own, z, c).start()
        @pl.when(z > 0)
        def _(): dn(s, own, z, c).start()
        yy(s, own, z, c).start()
    out_ref[own] = x_ref[...]
    for k in range(1, Z):
        for c in range(C):
            @pl.when(z - k >= 0)
            def _():
                zb = z - k; b = zb * 2 + y
                yy(blk(b, c), b, zb, c).wait_recv()
                @pl.when(z < Z - 1)
                def _(): up(blk(b, c), b, zb, c).start()
                yy(blk(b, c), b, zb, c).start()
            @pl.when(z + k <= Z - 1)
            def _():
                zb = z + k; b = zb * 2 + y
                yy(blk(b, c), b, zb, c).wait_recv()
                @pl.when(z > 0)
                def _(): dn(blk(b, c), b, zb, c).start()
                yy(blk(b, c), b, zb, c).start()
    for zb in range(Z):
        for c in range(C):
            b = zb * 2 + (1 - y)
            yy(blk(b, c), b, zb, c).wait_recv()
    for zb in range(Z):
        for c in range(C):
            b = zb * 2 + y
            yy(blk(b, c), b, zb, c).wait_send()
            @pl.when((z < Z - 1) & (zb <= z))
            def _(): up(blk(b, c), b, zb, c).wait_send()
            @pl.when((z > 0) & (zb >= z))
            def _(): dn(blk(b, c), b, zb, c).wait_send()


def ag(x, Z, C, cid=1):
    R, D = x.shape
    return pl.pallas_call(functools.partial(ag_kernel, Z, C),
        out_shape=jax.ShapeDtypeStruct((2 * Z, R, D), x.dtype),
        in_specs=[pl.BlockSpec(memory_space=pltpu.VMEM)], out_specs=pl.BlockSpec(memory_space=pltpu.VMEM),
        scratch_shapes=[pltpu.SemaphoreType.DMA((Z, C))] * 3 + [pltpu.SemaphoreType.DMA((2 * Z, C))],
        cost_estimate=pl.CostEstimate(flops=0, bytes_accessed=160_000_000, transcendentals=0),
        compiler_params=pltpu.CompilerParams(collective_id=cid, has_side_effects=True, vmem_limit_bytes=60 << 20))(x)


def rs_kernel(Z, C, p_ref, out_ref, ybuf, bbuf, abuf, ubuf, dbuf, ysem, usem, dsem, yr, br, ar):
    z = lax.axis_index("mlp"); y = lax.axis_index("head")
    R, _ = out_ref.shape; r = R // C
    enter(Z, z, y)
    def rows(c): return pl.ds(c * r, r)
    def yy(zb, c): return remote(p_ref.at[zb * 2 + 1 - y, rows(c)], ybuf.at[zb, rows(c)], ysem.at[zb, c], yr.at[zb, c], {"head": 1 - y})
    def up(zb, c): return remote(ubuf.at[zb, rows(c)], bbuf.at[zb, rows(c)], usem.at[zb, c], br.at[zb, c], {"mlp": z + 1})
    def dn(zb, c): return remote(dbuf.at[zb, rows(c)], abuf.at[zb, rows(c)], dsem.at[zb, c], ar.at[zb, c], {"mlp": z - 1})
    for k in range(Z - 1, -1, -1):
        for c in range(C):
            @pl.when(z + k <= Z - 1)
            def _(): yy(z + k, c).start()
            if k:
                @pl.when(z - k >= 0)
                def _(): yy(z - k, c).start()
    f = lambda v: v.astype(jnp.float32)
    def own(zb, c): return f(p_ref[zb * 2 + y, rows(c)]) + f(ybuf[zb, rows(c)])
    for k in range(Z - 1, 0, -1):
        for c in range(C):
            @pl.when(z + k <= Z - 1)
            def _():
                zb = z + k
                yy(zb, c).wait_recv()
                @pl.when(z > 0)
                def _():
                    up(zb, c).wait_recv()
                    ubuf[zb, rows(c)] = (own(zb, c) + f(bbuf[zb, rows(c)])).astype(ubuf.dtype)
                @pl.when(z == 0)
                def _():
                    ubuf[zb, rows(c)] = own(zb, c).astype(ubuf.dtype)
                up(zb, c).start()
            @pl.when(z - k >= 0)
            def _():
                zb = z - k
                yy(zb, c).wait_recv()
                @pl.when(z < Z - 1)
                def _():
                    dn(zb, c).wait_recv()
                    dbuf[zb, rows(c)] = (own(zb, c) + f(abuf[zb, rows(c)])).astype(dbuf.dtype)
                @pl.when(z == Z - 1)
                def _():
                    dbuf[zb, rows(c)] = own(zb, c).astype(dbuf.dtype)
                dn(zb, c).start()
    for c in range(C):
        yy(z, c).wait_recv()
        out_ref[rows(c)] = own(z, c)
        @pl.when(z > 0)
        def _():
            up(z, c).wait_recv()
            out_ref[rows(c)] += f(bbuf[z, rows(c)])
        @pl.when(z < Z - 1)
        def _():
            dn(z, c).wait_recv()
            out_ref[rows(c)] += f(abuf[z, rows(c)])
    for zb in range(Z):
        for c in range(C):
            yy(zb, c).wait_send()
            @pl.when(zb > z)
            def _(): up(zb, c).wait_send()
            @pl.when(zb < z)
            def _(): dn(zb, c).wait_send()


def rs(p, Z, C, cid=2):
    _, R, D = p.shape
    return pl.pallas_call(functools.partial(rs_kernel, Z, C),
        out_shape=jax.ShapeDtypeStruct((R, D), jnp.float32),
        in_specs=[pl.BlockSpec(memory_space=pltpu.VMEM)], out_specs=pl.BlockSpec(memory_space=pltpu.VMEM),
        scratch_shapes=[pltpu.VMEM((Z, R, D), p.dtype)] * 5 + [pltpu.SemaphoreType.DMA((Z, C))] * 6,
        cost_estimate=pl.CostEstimate(flops=0, bytes_accessed=160_000_000, transcendentals=0),
        compiler_params=pltpu.CompilerParams(collective_id=cid, has_side_effects=True, vmem_limit_bytes=60 << 20))(p)


def total_kernel(axes, x_ref, out_ref, *scratch):
    count = len(axes)
    slots, sums, send_sems, recv_sems = (scratch[i * count : (i + 1) * count] for i in range(4))
    barrier = pltpu.get_barrier_semaphore()
    for name, size in axes:
        me = lax.axis_index(name)
        for step in range(1, size):
            pl.semaphore_signal(
                barrier, inc=1, device_id={name: lax.rem(me + step, size)}, device_id_type=MESH
            )
    pl.semaphore_wait(barrier, sum(size - 1 for _, size in axes))
    current = x_ref
    for index, (name, size) in enumerate(axes):
        me = lax.axis_index(name)

        def copy(step):
            return remote(
                current,
                slots[index].at[me],
                send_sems[index].at[step],
                recv_sems[index].at[me],
                {name: lax.rem(me + step, size)},
            )

        def arrival(step):
            source = lax.rem(me + size - step, size)
            return remote(
                current,
                slots[index].at[source],
                send_sems[index].at[step],
                recv_sems[index].at[source],
                {name: lax.rem(me + step, size)},
            )

        for step in range(1, size):
            copy(step).start()
        slots[index][me] = current[...]
        for step in range(1, size):
            arrival(step).wait_recv()
        for step in range(1, size):
            copy(step).wait_send()
        total = slots[index][0]
        for slot in range(1, size):
            total = total + slots[index][slot]
        if index == count - 1:
            out_ref[...] = total
        else:
            sums[index][...] = total
            current = sums[index]


def total_over(values, axes, cid):
    shape = values.shape
    return pl.pallas_call(
        functools.partial(total_kernel, axes),
        out_shape=jax.ShapeDtypeStruct(shape, values.dtype),
        in_specs=[pl.BlockSpec(memory_space=pltpu.VMEM)],
        out_specs=pl.BlockSpec(memory_space=pltpu.VMEM),
        scratch_shapes=[pltpu.VMEM((size, *shape), values.dtype) for _, size in axes]
        + [pltpu.VMEM(shape, values.dtype) for _ in axes]
        + [pltpu.SemaphoreType.DMA((size,)) for _, size in axes] * 2,
        compiler_params=pltpu.CompilerParams(collective_id=cid, has_side_effects=True),
    )(values)


def gather_rows(rows, cid):
    full = ag(rows, lax.axis_size("mlp"), 2, cid)
    return full.reshape(-1, rows.shape[1])


def scatter_rows(partial, cid):
    levels = lax.axis_size("mlp")
    return rs(partial.reshape(2 * levels, -1, partial.shape[1]), levels, 2, cid)


def scatter_seq(gradient, dimension):
    part = lax.psum_scatter(gradient, "seq", scatter_dimension=dimension, tiled=True)
    return part.astype(jnp.float32)


def scaled_norm(values, norm_gain):
    return (
        values
        * lax.rsqrt(jnp.mean(values * values, axis=-1, keepdims=True) + norm_epsilon)
        * norm_gain
    )


def rotate(values, cosine_table, sine_table):
    middle = values.shape[-1] // 2
    front_half = values[..., :middle]
    back_half = values[..., middle:]
    return jnp.concatenate(
        [
            front_half * cosine_table - back_half * sine_table,
            back_half * cosine_table + front_half * sine_table,
        ],
        axis=-1,
    )


def rotary_tables(position, head_width):
    middle = head_width // 2
    frequency = jnp.exp(
        -(2.0 * jnp.arange(middle, dtype=jnp.float32) / head_width) * math.log(rope_base)
    )
    angles = position.astype(jnp.float32)[:, None] * frequency[None, :]
    return (jnp.cos(angles), jnp.sin(angles))


def document_layout(lengths, total_rows):
    end_points = jnp.cumsum(lengths)
    row_index = jnp.arange(total_rows, dtype=jnp.int32)
    passed = (row_index[:, None] >= end_points[None, :]).astype(jnp.int32)
    segment = jnp.sum(passed, axis=1)
    offset = jnp.sum(passed * lengths[None, :], axis=1)
    return (segment, row_index - offset)


def attention_classes(item_count, group_cols, query_cols, head_width):
    column = jnp.arange(item_count, dtype=jnp.int32) % group_cols
    return jnp.where(
        column < query_cols,
        0,
        jnp.where(
            column < query_cols + head_width,
            1,
            jnp.where(column < query_cols + 2 * head_width, 2, 3),
        ),
    ).astype(jnp.int32)


def forward_classes(item_count, group_cols):
    column = jnp.arange(item_count, dtype=jnp.int32) % group_cols
    return 4 + (column >= group_cols // 2).astype(jnp.int32)


def output_classes(item_count, group_rows, query_cols):
    row_index = jnp.arange(item_count, dtype=jnp.int32) % group_rows
    return 6 + (row_index >= query_cols).astype(jnp.int32)


def indicator_matrix(class_index):
    return (class_index[:, None] == jnp.arange(8, dtype=jnp.int32)[None, :]).astype(jnp.float32)


def kind_sums(matrix, kind_table, over_axis):
    return jnp.dot(
        jnp.sum(matrix * matrix, axis=over_axis), kind_table, precision=highest_precision
    )


def adam_terms(
    weight, gradient, first_moment, second_moment, correct_one, correct_two, decay_weight
):
    first_new = beta_one * first_moment + (1.0 - beta_one) * gradient
    second_new = beta_two * second_moment + (1.0 - beta_two) * gradient * gradient
    direction = (
        first_new / correct_one / (jnp.sqrt(second_new / correct_two) + adam_epsilon)
        + decay_weight * weight
    )
    return (first_new, second_new, direction)


def swiglu(gate_up_product):
    middle = gate_up_product.shape[-1] // 2
    return jax.nn.silu(gate_up_product[:, :middle]) * gate_up_product[:, middle:]


def contract_first(left, right):
    return lax.dot_general(
        left, right, (((0,), (0,)), ((), ())), preferred_element_type=jnp.float32
    )


def contract_last(left, right):
    return lax.dot_general(
        left, right, (((1,), (1,)), ((), ())), preferred_element_type=jnp.float32
    )


def visibility(segment, begin_row, end_row):
    row_index = jnp.arange(begin_row, end_row, dtype=jnp.int32)
    key_index = jnp.arange(end_row, dtype=jnp.int32)
    same_document = segment[begin_row:end_row, None] == segment[None, :end_row]
    return same_document & (key_index[None, :] <= row_index[:, None])


def block_scores(query_low, key_low, visible, begin_row, end_row, scaling):
    scores = (
        jnp.einsum(
            "qhd,kd->hqk",
            query_low[begin_row:end_row],
            key_low[:end_row],
            preferred_element_type=jnp.float32,
        )
        * scaling
    )
    return jnp.where(visible[None], scores, masked_score)


def shards(
    tokens,
    cotangent,
    attention_in,
    feedforward_in,
    projection_out,
    attention_mean,
    feedforward_mean,
    projection_mean,
    attention_power,
    feedforward_power,
    projection_power,
    gains,
    gain_mean,
    gain_power,
    document_lengths,
    step_count,
):
    own_rows = tokens.shape[0]
    model_width = tokens.shape[1]
    total_rows = own_rows * lax.axis_size(("mlp", "head"))
    head_width = (gains.shape[0] - 2 * model_width) // 2
    attention_cols = attention_in.shape[1]
    query_cols = attention_cols // 2 - head_width
    query_heads = query_cols // head_width
    feed_cols = feedforward_in.shape[1]
    output_rows = projection_out.shape[0]
    gain_one = gains[:model_width]
    gain_two = gains[model_width : 2 * model_width]
    gain_query = gains[2 * model_width : 2 * model_width + head_width]
    gain_key = gains[2 * model_width + head_width :]
    attention_lookup = indicator_matrix(
        attention_classes(attention_cols, attention_cols, query_cols, head_width)
    )
    forward_lookup = indicator_matrix(forward_classes(feed_cols, feed_cols))
    output_lookup = indicator_matrix(output_classes(output_rows, output_rows, query_cols))
    weight_local = (
        kind_sums(attention_in, attention_lookup, 0)
        + kind_sums(feedforward_in, forward_lookup, 0)
        + kind_sums(projection_out, output_lookup, 1)
    )
    attention_reduced, forward_reduced, output_reduced = (
        lax.all_gather(attention_in.astype(jnp.bfloat16), "seq", axis=0, tiled=True),
        lax.all_gather(feedforward_in.astype(jnp.bfloat16), "seq", axis=0, tiled=True),
        lax.all_gather(projection_out.astype(jnp.bfloat16), "seq", axis=1, tiled=True),
    )
    mixer_low = output_reduced[:query_cols]
    down_low = output_reduced[query_cols:]
    segment, position = document_layout(document_lengths[0], total_rows)
    cosine_table, sine_table = rotary_tables(position, head_width)
    inputs = tokens.astype(jnp.float32)
    normed_input, back_one = jax.vjp(scaled_norm, inputs, gain_one)
    normed_rows = gather_rows(normed_input.astype(jnp.bfloat16), 1)
    projected_rows = jnp.dot(normed_rows, attention_reduced, preferred_element_type=jnp.float32)
    query_rows = projected_rows[:, :query_cols].reshape(total_rows, query_heads, head_width)
    keys_raw = projected_rows[:, query_cols : query_cols + head_width]
    values_low = projected_rows[:, query_cols + head_width : query_cols + 2 * head_width].astype(
        jnp.bfloat16
    )
    gate_scores_raw = projected_rows[:, query_cols + 2 * head_width :]

    def prepare(query_in, key_in, query_gain, key_gain):
        query_out = rotate(
            scaled_norm(query_in, query_gain), cosine_table[:, None, :], sine_table[:, None, :]
        )
        key_out = rotate(scaled_norm(key_in, key_gain), cosine_table, sine_table)
        return (query_out, key_out)

    (query_rot, key_rot), back_prepare = jax.vjp(
        prepare, query_rows, keys_raw, gain_query, gain_key
    )
    query_low = query_rot.astype(jnp.bfloat16)
    key_low = key_rot.astype(jnp.bfloat16)
    block_rows = min(512, total_rows)
    block_count = total_rows // block_rows
    scaling = head_width ** (-0.5)
    pieces = []
    log_totals = []
    for block_index in range(block_count):
        begin_row = block_index * block_rows
        end_row = begin_row + block_rows
        visible = visibility(segment, begin_row, end_row)
        scores = block_scores(query_low, key_low, visible, begin_row, end_row, scaling)
        row_max = jnp.max(scores, axis=-1, keepdims=True)
        log_total = row_max + jnp.log(jnp.sum(jnp.exp(scores - row_max), axis=-1, keepdims=True))
        softmax_low = jnp.exp(scores - log_total).astype(jnp.bfloat16)
        pieces.append(
            jnp.einsum(
                "hqk,kd->qhd", softmax_low, values_low[:end_row], preferred_element_type=jnp.float32
            )
        )
        log_totals.append(log_total)
    attended_rows = jnp.concatenate(pieces, axis=0).reshape(total_rows, query_cols)
    gate_sigmoid = jax.nn.sigmoid(gate_scores_raw)
    gated_low = (attended_rows * gate_sigmoid).astype(jnp.bfloat16)
    attention_out = scatter_rows(
        jnp.dot(gated_low, mixer_low, preferred_element_type=jnp.float32).astype(jnp.bfloat16), 2
    )
    middle = inputs + attention_out
    normed_second, back_two = jax.vjp(scaled_norm, middle, gain_two)
    feed_rows = gather_rows(normed_second.astype(jnp.bfloat16), 3)
    gate_up_product = jnp.dot(feed_rows, forward_reduced, preferred_element_type=jnp.float32)
    activated, back_swiglu = jax.vjp(swiglu, gate_up_product)
    activated_low = activated.astype(jnp.bfloat16)
    cotangent_rows = lax.all_gather(cotangent, ("mlp", "head"), axis=0, tiled=True)
    delta_activated = contract_last(cotangent_rows, down_low)
    delta_gate_up = back_swiglu(delta_activated)[0].astype(jnp.bfloat16)
    down_gradient, feed_gradient, feed_delta_partial = lax.optimization_barrier(
        (
            contract_first(activated_low, cotangent_rows).astype(jnp.bfloat16),
            contract_first(feed_rows, delta_gate_up).astype(jnp.bfloat16),
            contract_last(delta_gate_up, forward_reduced).astype(jnp.bfloat16),
        )
    )
    feed_total = scatter_seq(feed_gradient, 0)
    down_total = scatter_seq(down_gradient, 1)
    delta_normed_two = scatter_rows(feed_delta_partial, 4)
    delta_middle_part, delta_gain_two = back_two(delta_normed_two)
    delta_middle = cotangent.astype(jnp.float32) + delta_middle_part
    branch_rows, feed_out_partial = lax.optimization_barrier(
        (
            gather_rows(delta_middle.astype(jnp.bfloat16), 5),
            jnp.dot(activated_low, down_low, preferred_element_type=jnp.float32).astype(
                jnp.bfloat16
            ),
        )
    )
    feed_out = lax.psum_scatter(
        feed_out_partial, ("mlp", "head"), scatter_dimension=0, tiled=True
    ).astype(jnp.float32)
    block_output = (middle + feed_out).astype(jnp.bfloat16)
    delta_gated = contract_last(branch_rows, mixer_low)
    mixer_total = scatter_seq(contract_first(gated_low, branch_rows).astype(jnp.bfloat16), 1)
    delta_attended = delta_gated * gate_sigmoid
    delta_logits = delta_gated * attended_rows * gate_sigmoid * (1.0 - gate_sigmoid)
    delta_attended_low = delta_attended.astype(jnp.bfloat16).reshape(
        total_rows, query_heads, head_width
    )
    query_deltas = []
    key_delta = jnp.zeros((total_rows, head_width), jnp.float32)
    value_delta = jnp.zeros((total_rows, head_width), jnp.float32)
    for block_index in range(block_count):
        begin_row = block_index * block_rows
        end_row = begin_row + block_rows
        visible = visibility(segment, begin_row, end_row)
        scores = block_scores(query_low, key_low, visible, begin_row, end_row, scaling)
        softmax_full = jnp.exp(scores - log_totals[block_index])
        softmax_low = softmax_full.astype(jnp.bfloat16)
        delta_rows = delta_attended_low[begin_row:end_row]
        delta_softmax = jnp.einsum(
            "qhd,kd->hqk", delta_rows, values_low[:end_row], preferred_element_type=jnp.float32
        )
        inner_sum = jnp.sum(softmax_full * delta_softmax, axis=-1, keepdims=True)
        delta_scores = (softmax_full * (delta_softmax - inner_sum)).astype(jnp.bfloat16)
        query_deltas.append(
            jnp.einsum(
                "hqk,kd->qhd", delta_scores, key_low[:end_row], preferred_element_type=jnp.float32
            )
            * scaling
        )
        key_delta = key_delta.at[:end_row].add(
            jnp.einsum(
                "hqk,qhd->kd",
                delta_scores,
                query_low[begin_row:end_row],
                preferred_element_type=jnp.float32,
            )
            * scaling
        )
        value_delta = value_delta.at[:end_row].add(
            jnp.einsum("hqk,qhd->kd", softmax_low, delta_rows, preferred_element_type=jnp.float32)
        )
    query_delta = jnp.concatenate(query_deltas, axis=0)
    query_back, key_back, delta_gain_query, delta_gain_key = back_prepare((query_delta, key_delta))
    delta_projected = jnp.concatenate(
        [query_back.reshape(total_rows, query_cols), key_back, value_delta, delta_logits], axis=1
    ).astype(jnp.bfloat16)
    attention_gradient, delta_partial = lax.optimization_barrier(
        (
            contract_first(normed_rows, delta_projected).astype(jnp.bfloat16),
            contract_last(delta_projected, attention_reduced).astype(jnp.bfloat16),
        )
    )
    attention_total = scatter_seq(attention_gradient, 0)
    delta_normed = scatter_rows(delta_partial, 6)
    delta_input_part, delta_gain_one = back_one(delta_normed)
    input_gradient = delta_middle + delta_input_part
    output_total = jnp.concatenate([mixer_total, down_total], axis=0)
    steps_done = step_count[0].astype(jnp.float32)
    correct_one = 1.0 - jnp.power(beta_one, steps_done)
    correct_two = 1.0 - jnp.power(beta_two, steps_done)
    mean_attention, power_attention, move_attention = adam_terms(
        attention_in,
        attention_total,
        attention_mean,
        attention_power,
        correct_one,
        correct_two,
        decay_rate,
    )
    mean_feedforward, power_feedforward, move_feed = adam_terms(
        feedforward_in,
        feed_total,
        feedforward_mean,
        feedforward_power,
        correct_one,
        correct_two,
        decay_rate,
    )
    mean_projection, power_projection, move_output = adam_terms(
        projection_out,
        output_total,
        projection_mean,
        projection_power,
        correct_one,
        correct_two,
        decay_rate,
    )
    update_local = (
        kind_sums(move_attention, attention_lookup, 0)
        + kind_sums(move_feed, forward_lookup, 0)
        + kind_sums(move_output, output_lookup, 1)
    )
    gain_local = jnp.concatenate([delta_gain_one, delta_gain_two, delta_gain_query, delta_gain_key])
    norm_local = jnp.concatenate([weight_local, update_local])
    packed = jnp.concatenate([gain_local, norm_local])
    packed_rows = -(-packed.shape[0] // 1024) * 8
    packed_total = total_over(
        jnp.pad(packed, (0, packed_rows * 128 - packed.shape[0])).reshape(packed_rows, 128),
        tuple((name, lax.axis_size(name)) for name in ("seq", "mlp", "head")),
        7,
    ).reshape(-1)
    gain_total = packed_total[: gain_local.shape[0]]
    norm_total = packed_total[gain_local.shape[0] : packed.shape[0]]
    weight_squares = norm_total[:8]
    update_squares = norm_total[8:]
    trust_ratio = jnp.sqrt(weight_squares) / jnp.sqrt(update_squares)
    attention_master = (
        attention_in
        - learn_rate
        * jnp.dot(attention_lookup, trust_ratio, precision=highest_precision)[None, :]
        * move_attention
    )
    feedforward_master = (
        feedforward_in
        - learn_rate
        * jnp.dot(forward_lookup, trust_ratio, precision=highest_precision)[None, :]
        * move_feed
    )
    projection_master = (
        projection_out
        - learn_rate
        * jnp.dot(output_lookup, trust_ratio, precision=highest_precision)[:, None]
        * move_output
    )
    mean_gains, power_gains, move_gains = adam_terms(
        gains, gain_total, gain_mean, gain_power, correct_one, correct_two, 0.0
    )
    gains_next = gains - learn_rate * move_gains
    matrix_norms = jnp.stack([jnp.sqrt(weight_squares), jnp.sqrt(update_squares)])
    return (
        block_output,
        input_gradient,
        attention_master,
        feedforward_master,
        projection_master,
        mean_attention,
        mean_feedforward,
        mean_projection,
        power_attention,
        power_feedforward,
        power_projection,
        attention_master.astype(jnp.bfloat16),
        feedforward_master.astype(jnp.bfloat16),
        projection_master.astype(jnp.bfloat16),
        gains_next,
        mean_gains,
        power_gains,
        matrix_norms,
    )


def solution(mesh):
    placed = (
        P(("seq", "mlp", "head"), None),
        P(("seq", "mlp", "head"), None),
        P("seq", ("mlp", "head")),
        P("seq", ("mlp", "head")),
        P(("mlp", "head"), "seq"),
        P("seq", ("mlp", "head")),
        P("seq", ("mlp", "head")),
        P(("mlp", "head"), "seq"),
        P("seq", ("mlp", "head")),
        P("seq", ("mlp", "head")),
        P(("mlp", "head"), "seq"),
        P(),
        P(),
        P(),
        P("seq", None),
        P(),
    )

    return jax.shard_map(
        shards,
        mesh=mesh,
        in_specs=placed,
        out_specs=(
            P(("seq", "mlp", "head"), None),
            P(("seq", "mlp", "head"), None),
            P("seq", ("mlp", "head")),
            P("seq", ("mlp", "head")),
            P(("mlp", "head"), "seq"),
            P("seq", ("mlp", "head")),
            P("seq", ("mlp", "head")),
            P(("mlp", "head"), "seq"),
            P("seq", ("mlp", "head")),
            P("seq", ("mlp", "head")),
            P(("mlp", "head"), "seq"),
            P("seq", ("mlp", "head")),
            P("seq", ("mlp", "head")),
            P(("mlp", "head"), "seq"),
            P(),
            P(),
            P(),
            P(),
        ),
        check_vma=False,
    )
```
